256 devices in a mesh: ea: 64 (over z, x, core), sa: 4 (over y).
Axes of the slice: x: 4, y: 4, z: 8, core: 2. Of those that a mesh axis runs over, the one named last changes fastest.
Arguments:
- expert_hidden: bfloat16 [256, 1792, 512], P('ea', 'sa'), may hold values from -6 to 6
- down_weight: bfloat16 [256, 512, 2048], P('ea'), may hold values from -0.25 to 0.25
- residual: bfloat16 [64, 512, 2048], P('ea', 'sa'), may hold values from -6 to 6
- expert_ids: int32 [64, 512, 10], P('ea', 'sa'), may hold values from 0 to 255, all different within a row; in each aligned block of 128 rows (0 to 127, 128 to 255, ..., all dimensions but the last counted through in order) at most 7 rows name the same one
- combine_weight: float32 [64, 512, 10], P('ea', 'sa'), may hold values from 0.05 to 0.3
- norm_gain: bfloat16 [2048], replicated, may hold values from 0.25 to 1.75
- value_weight: bfloat16 [2048, 2048], P('ea'), may hold values from -0.125 to 0.125
- queries: bfloat16 [64, 512, 1024], P('ea', 'sa'), may hold values from -6 to 6
- keys: bfloat16 [64, 512, 1024], P('ea', 'sa'), may hold values from -6 to 6
- log_decay: float32 [64, 512, 16], P('ea', 'sa'), may hold values from -1 to 0, as said below
- write_rate: float32 [64, 512, 16], P('ea', 'sa'), may hold values from 0.1 to 0.9
Outputs:
- head_out: bfloat16 [64, 512, 2048], P('ea', 'sa')
The draws below stay inside these ranges and needn't reach their ends.
Inputs may be any that keep to these rules, and one draw needn't show every extreme that they name: `expert_ids`: each row names 10 different experts; among the rows of one device (aligned blocks of 128 rows) no expert is named more than 7 times, a bound that some block reaches. `log_decay`: below zero.
All inputs are finite; a program needn't handle non-finite values.
Results may differ from the reference program's by a relative error of at most 0.0066.
Values may be sent and summed in bfloat16 or wider, within the bound.
No kernel may reach another device: no remote copies, remote signals or barrier semaphores. Data moves between devices by JAX's collectives and lax.ppermute only.
A program may use at most 128 MiB of HBM per device.

```python
import math
import jax
import jax.numpy as jnp
import numpy as np
from jax import lax

D = 2048
FF = 512
TOP = 10
HV = 16
HK = 8
DK = 128
DV = 128
TOK_DEV = 128
EXPERTS = 256
SEQS = 64
LEN = 512
CAP = 7
N_EA = 64
N_SA = 4


def draw_log_decay(key, part):
    k_fast, k_jitter, k_spots, k_drop = jax.random.split(key, 4)
    share = 0.5
    fast = jax.random.uniform(k_fast, (HV,)) < share
    slow_rate = 0.25 * math.log(10.0) / LEN
    base = jnp.where(fast, 1.0 / 40.0, slow_rate)
    jitter = jnp.exp(jax.random.uniform(k_jitter, (SEQS, LEN, HV), minval=-0.7, maxval=0.7))
    spots = jax.random.randint(k_spots, (SEQS, 2), 0, LEN)
    marked = jnp.any(jnp.arange(LEN)[None, :, None] == spots[:, None, :], axis=-1)
    drop = jnp.log(jax.random.uniform(k_drop, (SEQS, LEN), minval=0.5, maxval=0.8))
    final_result = -base[None, None, :] * jitter + jnp.where(marked, drop, 0.0)[:, :, None]
    return final_result.astype(jnp.float32)


def shard_levels(key, extent, pieces, smallest, top_value):
    level = 1.0
    for axis_at, parts in pieces:
        heights = jax.random.uniform(jax.random.fold_in(jax.random.fold_in(key, 6), axis_at), (parts,), jnp.float32, smallest / len(pieces), top_value / len(pieces))
        level = level * jnp.repeat(jnp.exp(heights), extent[axis_at] // parts).reshape((-1,) + (1,) * (len(extent) - 1 - axis_at))
    return level


def assign_block(own_key, own, number, rows, count, top, bound, lean):
    ranking = jax.random.permutation(own_key, count)
    crowded, ordinary = load_shares(count, rows * top, bound, lean, True), load_shares(count, rows * top, bound, lean, False)
    places = jnp.arange(count)

    def named(lengths, turn):
        used = int((lengths > 0).sum())
        fixed = max(1, used // 4)
        moved = fixed + (places - fixed + turn * (used - fixed)) % max(1, count - fixed)
        return jnp.zeros((count,), jnp.int32).at[ranking[jnp.where(places < fixed, places, moved)]].set(jnp.asarray(lengths, jnp.int32))

    lengths = jnp.where(number % 4 == 0, named(crowded, number // 4), named(ordinary, number - number // 4 - 1))
    mixed = jax.random.permutation(jax.random.fold_in(own, 3), count)
    source_of, receiver = mixed[0:count // 2 * 2:2], mixed[1:count // 2 * 2:2]
    room = jnp.minimum(lengths[source_of] - 1, bound - lengths[receiver]) // 2
    room = jnp.where((source_of == ranking[0]) | (receiver == ranking[0]) | (lengths[receiver] == 0), 0, jnp.maximum(room, 0))
    moved = jax.random.randint(jax.random.fold_in(own, 4), (count // 2,), 0, 1 << 20) % (room + 1)
    lengths = lengths.at[source_of].add(-moved).at[receiver].add(moved)
    members = jnp.searchsorted(jnp.cumsum(lengths), jnp.arange(rows * top), side="right").astype(jnp.int32)
    table = members.reshape(top, rows).T
    table = table[jax.random.permutation(jax.random.fold_in(own, 1), rows)]
    turn = jax.random.randint(jax.random.fold_in(own, 2), (rows, 1), 0, top)
    return jnp.take_along_axis(table, (jnp.arange(top)[None, :] + turn) % top, axis=1)


def load_shares(amount, total, limit, skew, full):
    portions = [(1 << 20) // math.isqrt(standing ** skew) + 1 for standing in range(1, amount + 1)]
    largest = limit if full else min(limit, max(-(-total // amount), total * portions[0] // sum(portions)))
    least = 1 if total - largest >= amount - 1 else 0
    given, spare = [largest] + [least] * (amount - 1), total - largest - least * (amount - 1)
    while spare > 0:
        movable = [i for i in range(1, amount) if given[i] < largest] or [i for i in range(1, amount) if given[i] < limit]
        pool, left = sum([portions[i] for i in movable]), spare
        for i in movable:
            extra = min(limit - given[i], max(1, left * portions[i] // pool), spare)
            given[i] = given[i] + extra
            spare = spare - extra
    return np.array(given)


def scatter_about(stream_key, extent, width, bound, cuts=(), kind=jnp.bfloat16):
    values = jax.random.normal(stream_key, extent, jnp.float32) * width
    if len(cuts) > 0:
        values = shard_levels(stream_key, extent, cuts, -0.22, 0.18) * values
    return jnp.clip(values, min=-bound, max=bound).astype(kind)


def setup_inputs(seed: int = 0) -> dict:
    key_of = jax.random.split(jax.random.key(seed), 12)
    expert_hidden = scatter_about(key_of[0], (EXPERTS, N_SA * N_EA * CAP, FF), 1.0, 6.0, ((0, 64), (1, 4)))
    down_weight = scatter_about(key_of[1], (EXPERTS, FF, D), FF ** -0.5, 0.25, ((0, 64),))
    residual = scatter_about(key_of[2], (SEQS, LEN, D), 1.0, 6.0, ((0, 64), (1, 4)))
    expert_ids_keys = jax.random.split(jax.random.fold_in(key_of[3], 1), SEQS * LEN // TOK_DEV)
    expert_ids_turns = jax.random.permutation(jax.random.fold_in(key_of[3], 3), SEQS * LEN // TOK_DEV)
    expert_ids = jax.vmap(lambda own, number: assign_block(jax.random.fold_in(key_of[3], 2), own, number, TOK_DEV, EXPERTS, TOP, CAP, 1))(expert_ids_keys, expert_ids_turns).reshape((SEQS, LEN, TOP))
    combine_weight = jnp.clip(0.05 + 0.25 * jax.random.uniform(key_of[4], (SEQS, LEN, TOP), jnp.float32) ** shard_levels(key_of[4], (SEQS, LEN, TOP), ((0, 64), (1, 4)), -0.2, 0.2), 0.05, 0.3)
    norm_gain = jnp.clip(1.0 + 0.15 * jax.random.normal(key_of[5], (D,), jnp.float32), 0.25, 1.75).astype(jnp.bfloat16)
    value_weight = scatter_about(key_of[6], (D, HV * DV), D ** -0.5, 0.125, ((0, 64),))
    queries = scatter_about(key_of[7], (SEQS, LEN, HK * DK), 1.0, 6.0, ((0, 64), (1, 4)))
    keys = scatter_about(key_of[8], (SEQS, LEN, HK * DK), 1.0, 6.0, ((0, 64), (1, 4)))
    log_decay = draw_log_decay(jax.random.fold_in(key_of[11], 71), 0)
    write_rate = jnp.clip(0.1 + 0.79999997 * jax.random.uniform(key_of[10], (SEQS, LEN, HV), jnp.float32) ** shard_levels(key_of[10], (SEQS, LEN, HV), ((0, 64), (1, 4)), -0.2, 0.2), 0.1, 0.9)
    return dict(expert_hidden=expert_hidden, down_weight=down_weight, residual=residual, expert_ids=expert_ids, combine_weight=combine_weight, norm_gain=norm_gain, value_weight=value_weight, queries=queries, keys=keys, log_decay=log_decay, write_rate=write_rate)


PRECISION_LEVEL = lax.Precision.HIGHEST

def block_slots(ids):
    onehot = (ids[:, :, None] == jnp.arange(EXPERTS, dtype=jnp.int32)[None, None, :]).astype(jnp.int32)
    counts = lax.optimization_barrier(jnp.sum(onehot, axis=1))
    prior = jnp.cumsum(counts, axis=0) - counts
    return lax.optimization_barrier(jnp.sum(onehot * prior[:, None, :], axis=-1)).astype(jnp.int32)

def unit_rows(field):
    return field * lax.rsqrt(lax.optimization_barrier(jnp.sum(field * field, axis=-1, keepdims=True)) + 1e-06)

def reference(expert_hidden, down_weight, residual, expert_ids, combine_weight, norm_gain, value_weight, queries, keys, log_decay, write_rate):
    down32 = down_weight.astype(jnp.float32)
    hidden5 = expert_hidden.reshape(EXPERTS, N_SA, N_EA, CAP, FF)
    per_seq = jnp.moveaxis(hidden5, 2, 0)

    def one_sequence(inputs):
        hid_seq, res_seq, ids_seq, weight_seq = inputs
        outs = jnp.einsum('ejcf,efd->ejcd', hid_seq.astype(jnp.float32), down32)
        flat = outs.reshape(EXPERTS * N_SA * CAP, D).astype(jnp.bfloat16)
        flat = lax.optimization_barrier(flat)
        ids_blocks = ids_seq.reshape(N_SA, TOK_DEV, TOP)
        slots = jax.vmap(block_slots)(ids_blocks)
        shard = jnp.arange(N_SA, dtype=jnp.int32)[:, None, None]
        rows = ((ids_blocks * N_SA + shard) * CAP + slots).reshape(LEN, TOP)
        picked = jnp.take(flat, rows, axis=0).astype(jnp.float32)
        moe = lax.optimization_barrier(jnp.sum(weight_seq[:, :, None] * picked, axis=1))
        return (res_seq.astype(jnp.float32) + moe).astype(jnp.bfloat16)
    stream = lax.map(one_sequence, (per_seq, residual, expert_ids, combine_weight))
    flow_float32 = lax.optimization_barrier(stream).astype(jnp.float32)
    normed = flow_float32 * lax.rsqrt(lax.optimization_barrier(jnp.mean(flow_float32 * flow_float32, axis=-1, keepdims=True)) + 1e-06) * norm_gain.astype(jnp.float32)
    normed = normed.astype(jnp.bfloat16)
    values = jnp.dot(normed.reshape(SEQS * LEN, D), value_weight, preferred_element_type=jnp.float32).astype(jnp.bfloat16)
    values = lax.optimization_barrier(values).astype(jnp.float32).reshape(SEQS, LEN, HV, DV)
    qn = unit_rows(queries.astype(jnp.float32).reshape(SEQS, LEN, HK, DK)) * DK ** (-0.5)
    kn = unit_rows(keys.astype(jnp.float32).reshape(SEQS, LEN, HK, DK))
    qn = jnp.repeat(qn, HV // HK, axis=2)
    kn = jnp.repeat(kn, HV // HK, axis=2)

    def advance(running_state, inputs):
        qt, kt, vt, at, bt = inputs
        alpha = jnp.exp(at)
        seen = jnp.einsum('shkv,shk->shv', running_state, kt, precision=PRECISION_LEVEL)
        delta = bt[..., None] * (vt - alpha[..., None] * seen)
        running_state = alpha[..., None, None] * running_state + kt[..., :, None] * delta[..., None, :]
        return (running_state, jnp.einsum('shkv,shk->shv', running_state, qt, precision=PRECISION_LEVEL))
    start = jnp.zeros((SEQS, HV, DK, DV), jnp.float32)
    inputs = (jnp.moveaxis(qn, 1, 0), jnp.moveaxis(kn, 1, 0), jnp.moveaxis(values, 1, 0), jnp.moveaxis(log_decay, 1, 0), jnp.moveaxis(write_rate, 1, 0))
    final, outs = lax.scan(advance, start, inputs)
    return jnp.moveaxis(outs, 0, 1).reshape(SEQS, LEN, HV * DV).astype(jnp.bfloat16)
```

```python
import jax
import jax.numpy as jnp
import numpy as np
from jax import lax
from jax.experimental import pallas as pl
from jax.experimental.pallas import tpu as pltpu
from jax.sharding import Mesh, PartitionSpec as P

HV = 16
HK = 8
DK = 128
DV = 128
CAP = 7
CHUNKS = (512, 512, 512, 512)
HIGHEST = lax.Precision.HIGHEST
F32 = jnp.float32
BF16 = jnp.bfloat16


def dot(a, b):
    return jnp.dot(a, b, preferred_element_type=F32)


def dot_high(a, b):
    return jnp.dot(a, b, preferred_element_type=F32, precision=HIGHEST)


def spread(array, axis):
    count = lax.axis_size(axis)
    return lax.all_to_all(
        jnp.broadcast_to(array[None], (count,) + array.shape),
        axis,
        split_axis=0,
        concat_axis=0,
        tiled=True,
    )


def produce_body(hidden_ref, weight_ref, out_ref):
    groups, _, rows, cols = out_ref.shape
    made = dot(hidden_ref[0], weight_ref[0])
    out_ref[:, 0] = made.reshape(groups, rows, cols).astype(BF16)


def produce(hidden, weight, start, cols, groups):
    experts, rows, units = hidden.shape
    block = cols
    while start % block:
        block //= 2
    return pl.pallas_call(
        produce_body,
        grid=(experts, cols // block),
        in_specs=[
            pl.BlockSpec((1, rows, units), lambda e, n: (e, 0, 0)),
            pl.BlockSpec((1, units, block), lambda e, n: (e, 0, start // block + n)),
        ],
        out_specs=pl.BlockSpec((groups, 1, rows // groups, block), lambda e, n: (0, e, 0, n)),
        out_shape=jax.ShapeDtypeStruct((groups, experts, rows // groups, cols), BF16),
        name="produce",
    )(hidden, weight)


def split_pair(x):
    high = x.astype(BF16)
    return jnp.concatenate([high, (x - high.astype(F32)).astype(BF16)], axis=1)


def maps_body(q_ref, k_ref, sum_col_ref, sum_row_ref, rate_col_ref, rate_row_ref, v_map_ref, s_map_ref):
    span = q_ref.shape[1]
    row = lax.broadcasted_iota(jnp.int32, (span, span), 0)
    col = lax.broadcasted_iota(jnp.int32, (span, span), 1)
    ident = (row == col).astype(F32)
    heads = v_map_ref.shape[1]
    share = heads // (q_ref.shape[2] // DK)
    for head in range(heads):
        at = (head // share) * DK
        q = q_ref[0, :, at : at + DK].astype(F32)
        k = k_ref[0, :, at : at + DK].astype(F32)
        q = q * lax.rsqrt(jnp.sum(q * q, axis=-1, keepdims=True) + 1e-06) * DK ** (-0.5)
        k = k * lax.rsqrt(jnp.sum(k * k, axis=-1, keepdims=True) + 1e-06)
        sum_col = sum_col_ref[0, :, head : head + 1]
        sum_row = sum_row_ref[0, head : head + 1, :]
        rate_col = rate_col_ref[0, :, head : head + 1]
        rate_row = rate_row_ref[0, head : head + 1, :]
        last = sum_row[:, span - 1 : span]
        growth = jnp.exp(sum_col)
        ratio = jnp.where(row >= col, jnp.exp(jnp.where(row >= col, sum_col - sum_row, 0.0)), 0.0)
        k_t = k.T
        lower = jnp.where(row > col, rate_col * ratio * dot_high(k, k_t), 0.0)
        scores = ratio * dot_high(q, k_t)
        small = jnp.where(row // 8 == col // 8, lower, 0.0)
        square = dot_high(small, small)
        fourth = dot_high(square, square)
        inverse = dot_high(ident - small, ident + square)
        inverse = dot_high(inverse, ident + fourth)
        size = 8
        while size < span:
            between = (row // (2 * size) == col // (2 * size)) & (row // size != col // size)
            inverse = inverse - dot_high(inverse, dot_high(jnp.where(between, lower, 0.0), inverse))
            size *= 2
        solve = inverse * rate_row
        seen = dot_high(solve, growth * k)
        tail_t = k_t * jnp.exp(last - sum_row)
        v_map_ref[0, head, :span, :] = split_pair(dot_high(scores, solve))
        v_map_ref[0, head, span:, :] = split_pair(dot_high(tail_t, solve))
        s_map_ref[0, head, :span, :] = split_pair(growth * q - dot_high(scores, seen))
        s_map_ref[0, head, span:, :] = split_pair(jnp.exp(last) * ident - dot_high(tail_t, seen))


def key_maps(q, k, sum_col, sum_row, rate_col, rate_row):
    blocks, span, width = q.shape
    heads = sum_row.shape[1]
    out = jax.ShapeDtypeStruct((blocks, heads, span + DK, 2 * span), BF16)

    def whole(array):
        return pl.BlockSpec((1,) + array.shape[1:], lambda n: (n,) + (0,) * (array.ndim - 1))

    args = (q, k, sum_col, sum_row, rate_col, rate_row)
    return pl.pallas_call(
        maps_body,
        grid=(blocks,),
        in_specs=[whole(a) for a in args],
        out_specs=[whole(out), whole(out)],
        out_shape=[out, out],
        name="key_maps",
    )(*args)


def emit_body(me_ref, v_ref, v_map_ref, s_map_ref, out_ref):
    blocks, span, _ = v_ref.shape
    heads = v_map_ref.shape[1]
    me = me_ref[0]
    states = [None] * heads
    for n in range(blocks):
        at = lax.rem(me - n + blocks, blocks)
        for head in range(heads):
            lanes = slice(head * DV, (head + 1) * DV)
            v = v_ref[at, :, lanes]
            made = dot(v_map_ref[n, head], jnp.concatenate([v, v], axis=0))
            if n > 0:
                state = states[head]
                high = state.astype(BF16)
                low = (state - high.astype(F32)).astype(BF16)
                maps = s_map_ref[n, head]
                made = made + dot(maps, jnp.concatenate([high, high], axis=0))
                made = made + dot(maps[:, :DK], low)
            out_ref[n, :, lanes] = made[:span].astype(BF16)
            states[head] = made[span:]


def emit(me, values, v_map, s_map):
    return pl.pallas_call(
        emit_body,
        in_specs=[pl.BlockSpec(memory_space=pltpu.SMEM)] + [pl.BlockSpec(memory_space=pltpu.VMEM)] * 3,
        out_specs=pl.BlockSpec(memory_space=pltpu.VMEM),
        out_shape=jax.ShapeDtypeStruct(values.shape, BF16),
        name="emit",
    )(me, values, v_map, s_map)


def combine_matrix(ids, weights, base, experts, groups):
    count, tokens, _ = ids.shape
    local = base + jnp.arange(experts, dtype=F32)
    named = ids[..., None] == local
    counts = jnp.sum(named.astype(F32), axis=2)
    dense = jnp.sum(jnp.where(named, weights[..., None], 0.0), axis=2).astype(BF16)
    earlier = (
        lax.broadcasted_iota(jnp.int32, (tokens, tokens), 0)
        > lax.broadcasted_iota(jnp.int32, (tokens, tokens), 1)
    ).astype(BF16)
    prior = jnp.einsum("tp,zpe->zte", earlier, counts.astype(BF16), preferred_element_type=F32)
    rows = experts * count * CAP
    each = experts // groups
    at = lax.broadcasted_iota(jnp.int32, (experts, rows), 1)
    owner = at // (rows // groups) * each + at % (rows // groups) // (count * CAP)
    pick = (owner == lax.broadcasted_iota(jnp.int32, (experts, rows), 0)).astype(BF16)
    prior_rows = jnp.einsum("zte,er->ztr", prior.astype(BF16), pick, preferred_element_type=F32)
    dense_rows = jnp.einsum("zte,er->ztr", dense, pick, preferred_element_type=F32)
    at = lax.broadcasted_iota(jnp.int32, (count, 1, rows), 2)
    mine = at % (count * CAP) // CAP == lax.broadcasted_iota(jnp.int32, (count, 1, rows), 0)
    hit = mine & (prior_rows == (at % CAP).astype(F32))
    return jnp.where(hit, dense_rows, 0.0).astype(BF16)


def on_device(
    expert_hidden,
    down_weight,
    residual,
    expert_ids,
    combine_weight,
    norm_gain,
    value_weight,
    queries,
    keys,
    log_decay,
    write_rate,
):
    n_z, n_x, n_c, n_sa = (lax.axis_size(a) for a in ("z", "x", "c", "sa"))
    n_xc = n_x * n_c
    exp_dev, units, width = down_weight.shape
    tokens = residual.shape[1]
    own = width // n_sa
    sa = lax.axis_index("sa")

    rows = expert_hidden.shape[1]
    at = np.arange(rows).reshape(n_z, n_xc, CAP).transpose(1, 0, 2).reshape(rows)
    order = jnp.asarray((at[:, None] == np.arange(rows)[None, :]), dtype=BF16)
    hidden = jnp.einsum(
        "pr,erf->epf", order, expert_hidden, preferred_element_type=F32
    ).astype(BF16)

    table = jnp.concatenate([expert_ids[0].astype(F32), combine_weight[0]], axis=1).T
    tables = spread(table, "z")
    top = expert_ids.shape[2]
    tables = tables.transpose(0, 2, 1)
    combine = combine_matrix(
        tables[..., :top],
        tables[..., top:],
        (lax.axis_index("z") * (n_xc * exp_dev)).astype(F32),
        n_xc * exp_dev,
        n_xc,
    ).reshape(n_z * tokens, n_xc * exp_dev * n_z * CAP)

    part = lax.dynamic_slice_in_dim(value_weight, sa * own, own, axis=1)
    part = spread(part, "z")
    part = spread(part, "x")
    part = spread(part, "c")
    projection = part.transpose(2, 1, 0, 3, 4).reshape(width, own)

    def to_heads(array):
        return lax.all_to_all(
            array.reshape(tokens, n_sa, -1).transpose(1, 0, 2),
            "sa",
            split_axis=0,
            concat_axis=0,
            tiled=True,
        )

    heads = HV // n_sa
    qk = to_heads(
        jnp.concatenate(
            [queries[0].reshape(tokens, n_sa, -1), keys[0].reshape(tokens, n_sa, -1)], axis=2
        )
    )
    rates = jnp.concatenate(
        [log_decay[0].T.reshape(n_sa, heads, tokens), write_rate[0].T.reshape(n_sa, heads, tokens)],
        axis=1,
    )
    rates = lax.all_to_all(rates, "sa", split_axis=0, concat_axis=0, tiled=True)
    until = (
        lax.broadcasted_iota(jnp.int32, (tokens, tokens), 0)
        <= lax.broadcasted_iota(jnp.int32, (tokens, tokens), 1)
    ).astype(F32)
    sum_row = jnp.einsum("nhp,pt->nht", rates[:, :heads], until, precision=HIGHEST)
    rate_row = rates[:, heads:]
    half = qk.shape[2] // 2
    v_map, s_map = key_maps(
        qk[..., :half],
        qk[..., half:],
        sum_row.transpose(0, 2, 1),
        sum_row,
        rate_row.transpose(0, 2, 1),
        rate_row,
    )

    start = 0
    total = jnp.zeros((n_sa * tokens, own), F32)
    squares = jnp.zeros((n_sa, tokens, 1), F32)
    for cols in CHUNKS:
        made = produce(hidden, down_weight, start, cols, n_xc)
        made = lax.all_to_all(made, ("x", "c"), split_axis=0, concat_axis=0, tiled=True)
        sums = dot(combine, made.reshape(-1, cols)).astype(BF16).reshape(n_z, tokens, cols)
        sums = lax.all_to_all(sums, "z", split_axis=0, concat_axis=0, tiled=True)
        stream = (
            residual[0, :, start : start + cols].astype(F32) + jnp.sum(sums.astype(F32), axis=0)
        ).astype(BF16)
        streams = [stream] + [
            lax.ppermute(stream, "sa", [(i, (i + s) % n_sa) for i in range(n_sa)])
            for s in range(1, n_sa)
        ]
        streams = jnp.stack(streams).astype(F32)
        squares += jnp.sum(streams * streams, axis=-1, keepdims=True)
        scaled = (streams * norm_gain[start : start + cols].astype(F32)).astype(BF16)
        total += dot(scaled.reshape(n_sa * tokens, cols), projection[start : start + cols])
        start += cols
    values = (
        total.reshape(n_sa, tokens, own) * lax.rsqrt(squares / width + 1e-06)
    ).astype(BF16)
    out = emit(sa[None], values, v_map, s_map)
    out = lax.all_to_all(out, "sa", split_axis=0, concat_axis=0, tiled=True)
    return out.transpose(1, 0, 2).reshape(1, tokens, width)


def solution(mesh):
    fine = Mesh(mesh.devices.reshape(8, 4, 2, 4), ("z", "x", "c", "sa"))
    ea = ("z", "x", "c")
    return jax.shard_map(
        on_device,
        mesh=fine,
        in_specs=(
            P(ea, "sa", None),
            P(ea, None, None),
            P(ea, "sa", None),
            P(ea, "sa", None),
            P(ea, "sa", None),
            P(),
            P(ea, None),
            P(ea, "sa", None),
            P(ea, "sa", None),
            P(ea, "sa", None),
            P(ea, "sa", None),
        ),
        out_specs=P(ea, "sa", None),
        check_vma=False,
    )
```

```python
import jax
import jax.numpy as jnp
from jax import lax
from jax.experimental import pallas as pl
from jax.experimental.pallas import tpu as pltpu
from jax.sharding import Mesh, PartitionSpec as P

HV = 16
DK = 128
DV = 128
CAP = 7
CHUNKS = (768, 640, 640)
HIGHEST = lax.Precision.HIGHEST
F32 = jnp.float32
BF16 = jnp.bfloat16
WHOLE = pl.BlockSpec(memory_space=pltpu.VMEM)
SCALARS = pl.BlockSpec(memory_space=pltpu.SMEM)


def dot(a, b):
    return jnp.dot(a, b, preferred_element_type=F32)


def halves(x):
    high = x.astype(BF16)
    return high, (x - high.astype(F32)).astype(BF16)


def dot_split(a, b):
    a_high, a_low = halves(a)
    b_high, b_low = halves(b)
    both = jnp.concatenate([a_high, a_low], axis=1)
    return dot(both, jnp.concatenate([b_high, b_high], axis=0)) + dot(a_high, b_low)


def shifted(array, axis, by):
    names = axis if isinstance(axis, tuple) else (axis,)
    count = 1
    for name in names:
        count *= lax.axis_size(name)
    return lax.ppermute(array, axis, [(i, (i + by) % count) for i in range(count)])


def gathered(array, axis, sign=1):
    held, by = array[None], 1
    while by < lax.axis_size(axis):
        held = jnp.concatenate([held, shifted(held, axis, sign * by)], axis=0)
        by *= 2
    return held


def thirds(x):
    pieces = []
    for _ in range(3):
        piece = lax.reduce_precision(x, 8, 7)
        pieces.append(piece.astype(BF16))
        x = x - piece
    return pieces


def ordered_hidden(expert_hidden, n_z, n_xc):
    experts, rows, _ = expert_hidden.shape
    half = n_z // 2
    used = half * CAP
    padded = n_xc * 2 * 32
    at = lax.broadcasted_iota(jnp.int32, (experts, padded, 1), 1)
    odd = lax.broadcasted_iota(jnp.int32, (experts, padded, 1), 0) % 2
    inner = at % 32 - odd * (32 - used)
    z = (lax.axis_index("z") + at // 32 % 2 * half + inner // CAP) % n_z
    xc = at // 64
    source = jnp.where((inner >= 0) & (inner < used), (z * n_xc + xc) * CAP + inner % CAP, -1)
    order = (source == lax.broadcasted_iota(jnp.int32, (1, 1, rows), 2)).astype(BF16)
    return jnp.einsum(
        "epr,erf->epf", order, expert_hidden, preferred_element_type=F32
    ).astype(BF16)


def produce_body(hidden_ref, weight_ref, out_ref):
    experts = hidden_ref.shape[0]
    made = [dot(hidden_ref[e], weight_ref[e]) for e in range(experts)]
    for group in range(out_ref.shape[0]):
        for half in range(2):
            at = (group * 2 + half) * 32
            pieces = []
            for e in range(0, experts, 2):
                a, b = made[e][at : at + 32], made[e + 1][at : at + 32]
                pieces += [a[:24], a[24:] + b[:8], b[8:]]
            rows = jnp.concatenate(pieces, axis=0)
            span = rows.shape[0]
            out_ref[group, half * span : (half + 1) * span, :] = rows.astype(BF16)


def produce(hidden, weight, start, cols, n_xc):
    experts, rows, units = hidden.shape
    block = 128
    while start % (2 * block) == 0 and cols % (2 * block) == 0 and block < 256:
        block *= 2
    sent = experts * 28 * 2
    return pl.pallas_call(
        produce_body,
        grid=(cols // block,),
        in_specs=[
            pl.BlockSpec((experts, rows, units), lambda n: (0, 0, 0)),
            pl.BlockSpec((experts, units, block), lambda n: (0, 0, start // block + n)),
        ],
        out_specs=pl.BlockSpec((n_xc, sent, block), lambda n: (0, 0, n)),
        out_shape=jax.ShapeDtypeStruct((n_xc, sent, cols), BF16),
        name="produce",
    )(hidden, weight)


def combine_matrix(tables, top, experts_of, n_xc):
    n_z, tokens, _ = tables.shape
    half = n_z // 2
    experts = experts_of * n_xc
    ids, weights = tables[..., :top], tables[..., top:]
    base = (lax.axis_index("z") * experts).astype(F32)
    named = ids[..., None] == base + jnp.arange(experts, dtype=F32)
    counts = jnp.sum(named.astype(F32), axis=2)
    dense = jnp.sum(jnp.where(named, weights[..., None], 0.0), axis=2).astype(BF16)
    earlier = (
        lax.broadcasted_iota(jnp.int32, (tokens, tokens), 0)
        > lax.broadcasted_iota(jnp.int32, (tokens, tokens), 1)
    ).astype(BF16)
    prior = jnp.einsum("tp,zpe->zte", earlier, counts.astype(BF16), preferred_element_type=F32)
    each = experts_of * half * CAP
    rows = each * n_xc
    at = lax.broadcasted_iota(jnp.int32, (experts, rows), 1)
    owner = at // (half * CAP)
    pick = (owner == lax.broadcasted_iota(jnp.int32, (experts, rows), 0)).astype(BF16)
    prior_rows = jnp.einsum("zte,er->ztr", prior.astype(BF16), pick, preferred_element_type=F32)
    dense_rows = jnp.einsum("zte,er->ztr", dense, pick, preferred_element_type=F32)
    at = lax.broadcasted_iota(jnp.int32, (n_z, 1, rows), 2)
    mine = at % (half * CAP) // CAP == lax.broadcasted_iota(jnp.int32, (n_z, 1, rows), 0) % half
    hit = mine & (prior_rows == (at % CAP).astype(F32))
    return jnp.where(hit, dense_rows, 0.0).astype(BF16).reshape(2, half * tokens, rows)


def combine_body(combine_ref, got_ref, *outs):
    half = len(outs) // 2
    n_xc, rows, cols = got_ref.shape
    rows //= 2
    tokens = outs[0].shape[0]
    for h in range(2):
        filled = got_ref[:, h * rows : (h + 1) * rows, :].reshape(n_xc * rows, cols)
        sums = dot(combine_ref[h], filled)
        for z in range(half):
            outs[h * half + z][...] = sums[z * tokens : (z + 1) * tokens].astype(BF16)


def combine_rows(combine, got, n_z):
    tokens = combine.shape[1] * 2 // n_z
    cols = got.shape[2]
    return pl.pallas_call(
        combine_body,
        in_specs=[WHOLE, WHOLE],
        out_specs=[WHOLE] * n_z,
        out_shape=[jax.ShapeDtypeStruct((tokens, cols), BF16)] * n_z,
        name="combine",
    )(combine, got)


def sum_rounded(*parts):
    total = parts[0].astype(F32)
    for part in parts[1:]:
        total = total + part.astype(F32)
    return total.astype(BF16)


def sum_over_z(parts, upward):
    up = shifted(parts[3], "z", 1)
    down = shifted(parts[5], "z", -1)
    far = shifted(parts[4], "z", 2 if upward else -2)
    near = [shifted(parts[1], "z", 1), shifted(parts[7], "z", -1)]
    plus = sum_rounded(*([parts[2], up] + ([far] if upward else [])))
    minus = sum_rounded(*([parts[6], down] + ([] if upward else [far])))
    return [parts[0]] + near + [shifted(plus, "z", 2), shifted(minus, "z", -2)]


def maps_body(q_ref, k_ref, sum_col_ref, sum_row_ref, rate_col_ref, rate_row_ref, v_map_ref, s_map_ref):
    span = q_ref.shape[1]
    row = lax.broadcasted_iota(jnp.int32, (span, span), 0)
    col = lax.broadcasted_iota(jnp.int32, (span, span), 1)
    ident = (row == col).astype(F32)
    heads = v_map_ref.shape[1]
    share = heads // (q_ref.shape[2] // DK)
    every = range(heads)
    queries, keys, keys_t, met = [], [], [], []
    for at in range(0, q_ref.shape[2], DK):
        q = q_ref[0, :, at : at + DK].astype(F32)
        k = k_ref[0, :, at : at + DK].astype(F32)
        q = q * lax.rsqrt(jnp.sum(q * q, axis=-1, keepdims=True) + 1e-06) * DK ** (-0.5)
        k = k * lax.rsqrt(jnp.sum(k * k, axis=-1, keepdims=True) + 1e-06)
        queries.append(q)
        keys.append(k)
        keys_t.append(k.T)
        met.append(dot_split(jnp.concatenate([k, q], axis=0), keys_t[-1]))
    lower, scores, inverse = [], [], []
    for head in every:
        away = sum_col_ref[0, :, head : head + 1] - sum_row_ref[0, head : head + 1, :]
        ratio = jnp.where(row >= col, jnp.exp(jnp.where(row >= col, away, 0.0)), 0.0)
        pair = met[head // share]
        rate = rate_col_ref[0, :, head : head + 1]
        lower.append(jnp.where(row > col, rate * ratio * pair[:span], 0.0))
        scores.append(ratio * pair[span:])
    small = [jnp.where(row // 8 == col // 8, lower[h], 0.0) for h in every]
    square = [dot_split(small[h], small[h]) for h in every]
    inverse = [dot_split(ident - small[h], ident + square[h]) for h in every]
    fourth = [dot_split(square[h], square[h]) for h in every]
    inverse = [dot_split(inverse[h], ident + fourth[h]) for h in every]
    size = 8
    while size < span:
        between = (row // (2 * size) == col // (2 * size)) & (row // size != col // size)
        moved = [dot_split(jnp.where(between, lower[h], 0.0), inverse[h]) for h in every]
        inverse = [inverse[h] - dot_split(inverse[h], moved[h]) for h in every]
        size *= 2
    v_maps = []
    for head in every:
        sum_row = sum_row_ref[0, head : head + 1, :]
        tail = keys_t[head // share] * jnp.exp(sum_row[:, span - 1 : span] - sum_row)
        solve = inverse[head] * rate_row_ref[0, head : head + 1, :]
        v_maps.append(dot_split(jnp.concatenate([scores[head], tail], axis=0), solve))
        v_map_ref[0, head] = jnp.concatenate(halves(v_maps[-1]), axis=1)
    for head in every:
        growth = jnp.exp(sum_col_ref[0, :, head : head + 1])
        whole = jnp.exp(sum_row_ref[0, head : head + 1, span - 1 : span])
        fixed = jnp.concatenate([growth * queries[head // share], whole * ident], axis=0)
        s_map = fixed - dot_split(v_maps[head], growth * keys[head // share])
        s_map_ref[0, head] = jnp.concatenate(halves(s_map), axis=1)


def key_maps(*args):
    blocks, span, _ = args[0].shape
    heads = args[3].shape[1]
    out = jax.ShapeDtypeStruct((blocks, heads, span + DK, 2 * span), BF16)

    def whole(array):
        return pl.BlockSpec((1,) + array.shape[1:], lambda n: (n,) + (0,) * (array.ndim - 1))

    return pl.pallas_call(
        maps_body,
        grid=(blocks,),
        in_specs=[whole(a) for a in args],
        out_specs=[whole(out), whole(out)],
        out_shape=[out, out],
        name="key_maps",
    )(*args)


def order_body(at_ref, part_ref, out_ref):
    n_c, n_x, n_z, rows, _ = part_ref.shape
    for z in range(n_z):
        for x in range(n_x):
            for c in range(n_c):
                place = ((z * n_x + x) * n_c + c) * rows
                out_ref[place : place + rows, :] = part_ref[
                    lax.rem(at_ref[2] - c + n_c, n_c),
                    lax.rem(at_ref[1] - x + n_x, n_x),
                    lax.rem(at_ref[0] - z + n_z, n_z),
                ]


def finish_body(n_sa, me_ref, gain_ref, weight_ref, v_map_ref, s_map_ref, *refs):
    streams, outs = refs[: -n_sa - 2], refs[-n_sa - 2 : -2]
    normed_ref, head_ref = refs[-2:]
    tokens, own = outs[0].shape
    heads = v_map_ref.shape[1]
    width = normed_ref.shape[1]
    me = me_ref[0]
    gain = gain_ref[...].astype(F32)
    for s in range(n_sa):
        stream = jnp.concatenate([a[...] for a in streams[s::n_sa]], axis=1).astype(F32)
        scale = lax.rsqrt(jnp.sum(stream * stream, axis=-1, keepdims=True) / width + 1e-06)
        normed_ref[s * tokens : (s + 1) * tokens, :] = (stream * scale * gain).astype(BF16)
    made = dot(normed_ref[...], weight_ref[...]).astype(BF16)
    for s in range(n_sa):
        head_ref[lax.rem(me - s + n_sa, n_sa)] = made[s * tokens : (s + 1) * tokens]
    states = [None] * heads
    for n in range(n_sa):
        at = lax.rem(me - n + n_sa, n_sa)
        for head in range(heads):
            lanes = slice(head * DV, (head + 1) * DV)
            v = head_ref[n, :, lanes]
            out = dot(v_map_ref[at, head], jnp.concatenate([v, v], axis=0))
            if n > 0:
                high, low = halves(states[head])
                maps = s_map_ref[at, head]
                out = out + dot(maps, jnp.concatenate([high, high], axis=0))
                out = out + dot(maps[:, :DK], low)
            head_ref[n, :, lanes] = out[:tokens].astype(BF16)
            states[head] = out[tokens:]
    for s in range(n_sa):
        outs[s][...] = head_ref[lax.rem(me + s, n_sa)]


def finish(me, gain, weight, v_map, s_map, streams, n_sa):
    tokens = streams[0].shape[0]
    width, own = weight.shape

    def body(*refs):
        finish_body(n_sa, *refs)

    return pl.pallas_call(
        body,
        in_specs=[SCALARS] + [WHOLE] * (4 + len(streams)),
        out_specs=[WHOLE] * n_sa,
        out_shape=[jax.ShapeDtypeStruct((tokens, own), BF16)] * n_sa,
        scratch_shapes=[
            pltpu.VMEM((n_sa * tokens, width), BF16),
            pltpu.VMEM((n_sa, tokens, own), BF16),
        ],
        name="finish",
    )(me, gain, weight, v_map, s_map, *streams)


def place_body(me_ref, *refs):
    got, out_ref = refs[:-1], refs[-1]
    own = got[0].shape[1]
    for s, ref in enumerate(got):
        at = lax.rem(me_ref[0] - s + len(got), len(got))
        out_ref[:, pl.ds(pl.multiple_of(at * own, own), own)] = ref[...]


def on_device(
    expert_hidden,
    down_weight,
    residual,
    expert_ids,
    combine_weight,
    norm_gain,
    value_weight,
    queries,
    keys,
    log_decay,
    write_rate,
):
    n_z, n_x, n_c, n_sa = (lax.axis_size(a) for a in ("z", "x", "c", "sa"))
    n_xc = n_x * n_c
    exp_dev, _, width = down_weight.shape
    tokens = residual.shape[1]
    top = expert_ids.shape[2]
    own = width // n_sa
    heads = HV // n_sa
    sa = lax.axis_index("sa")
    me = sa[None]

    hidden = ordered_hidden(expert_hidden, n_z, n_xc)

    table = jnp.concatenate([expert_ids[0].astype(F32), combine_weight[0]], axis=1).T
    tables = gathered(table, "z", -1)
    combine = combine_matrix(tables.transpose(0, 2, 1), top, exp_dev, n_xc)

    part = lax.dynamic_slice_in_dim(value_weight, sa * own, own, axis=1)
    for axis in ("z", "x", "c"):
        part = gathered(part, axis)
    place = jnp.stack([lax.axis_index(a) for a in ("z", "x", "c")])
    projection = pl.pallas_call(
        order_body,
        in_specs=[SCALARS, WHOLE],
        out_specs=WHOLE,
        out_shape=jax.ShapeDtypeStruct((width, own), BF16),
        name="order",
    )(place, part)

    def by_group(array):
        return array[0].reshape(tokens, n_sa, -1).transpose(1, 0, 2)

    rates = jnp.concatenate(
        [log_decay[0].T.reshape(n_sa, heads, tokens), write_rate[0].T.reshape(n_sa, heads, tokens)],
        axis=1,
    )
    rates = jnp.stack(thirds(rates), axis=1).reshape(n_sa, -1, own)
    extra = rates.shape[1]
    rates = jnp.pad(rates, ((0, 0), (0, -extra % 8), (0, 0)))
    sent = jnp.concatenate([by_group(queries), by_group(keys)], axis=2)
    sent = jnp.concatenate([sent, rates], axis=1)
    qk = []
    for s in range(n_sa):
        piece = lax.dynamic_index_in_dim(sent, (sa + s) % n_sa, keepdims=False)
        qk.append(shifted(piece, "sa", s) if s else piece)
    qk = jnp.stack(qk)
    rates = qk[:, tokens : tokens + extra].reshape(n_sa, 3, 2 * heads, tokens).astype(F32)
    rates = rates[:, 0] + rates[:, 1] + rates[:, 2]
    qk = qk[:, :tokens]
    until = (
        lax.broadcasted_iota(jnp.int32, (tokens, tokens), 0)
        <= lax.broadcasted_iota(jnp.int32, (tokens, tokens), 1)
    ).astype(F32)
    sum_row = jnp.einsum("nhp,pt->nht", rates[:, :heads], until, precision=HIGHEST)
    rate_row = rates[:, heads:]
    half = qk.shape[2] // 2
    v_map, s_map = key_maps(
        qk[..., :half],
        qk[..., half:],
        sum_row.transpose(0, 2, 1),
        sum_row,
        rate_row.transpose(0, 2, 1),
        rate_row,
    )

    start = 0
    streams = []
    for number, cols in enumerate(CHUNKS):
        made = produce(hidden, down_weight, start, cols, n_xc)
        got = lax.all_to_all(made, ("x", "c"), split_axis=0, concat_axis=0, tiled=True)
        parts = combine_rows(combine, got, n_z)
        parts = sum_over_z(parts, number % 2 == 0)
        stream = sum_rounded(residual[0, :, start : start + cols], *parts)
        streams += [stream] + [shifted(stream, "sa", s) for s in range(1, n_sa)]
        start += cols
    outs = finish(me, norm_gain[None], projection, v_map, s_map, streams, n_sa)
    outs = [outs[0]] + [shifted(outs[s], "sa", s) for s in range(1, n_sa)]
    out = pl.pallas_call(
        place_body,
        in_specs=[SCALARS] + [WHOLE] * n_sa,
        out_specs=WHOLE,
        out_shape=jax.ShapeDtypeStruct((tokens, width), BF16),
        name="place",
    )(me, *outs)
    return out[None]


def solution(mesh):
    fine = Mesh(mesh.devices.reshape(8, 4, 2, 4), ("z", "x", "c", "sa"))
    ea = ("z", "x", "c")
    return jax.shard_map(
        on_device,
        mesh=fine,
        in_specs=(
            P(ea, "sa", None),
            P(ea, None, None),
            P(ea, "sa", None),
            P(ea, "sa", None),
            P(ea, "sa", None),
            P(),
            P(ea, None),
            P(ea, "sa", None),
            P(ea, "sa", None),
            P(ea, "sa", None),
            P(ea, "sa", None),
        ),
        out_specs=P(ea, "sa", None),
        check_vma=False,
    )
```

```python
import jax
import jax.numpy as jnp
from jax import lax
from jax.experimental import pallas as pl
from jax.experimental.pallas import tpu as pltpu
from jax.sharding import Mesh, PartitionSpec as P

HV = 16
DK = 128
DV = 128
CAP = 7
CHUNKS = (768, 768, 512)
HIGHEST = lax.Precision.HIGHEST
F32 = jnp.float32
BF16 = jnp.bfloat16
WHOLE = pl.BlockSpec(memory_space=pltpu.VMEM)
SCALARS = pl.BlockSpec(memory_space=pltpu.SMEM)


def dot(a, b):
    return jnp.dot(a, b, preferred_element_type=F32)


def halves(x):
    high = x.astype(BF16)
    return high, (x - high.astype(F32)).astype(BF16)


def dot_split(a, b):
    a_high, a_low = halves(a)
    b_high, b_low = halves(b)
    both = jnp.concatenate([a_high, a_low], axis=1)
    return dot(both, jnp.concatenate([b_high, b_high], axis=0)) + dot(a_high, b_low)


def shifted(array, axis, by):
    names = axis if isinstance(axis, tuple) else (axis,)
    count = 1
    for name in names:
        count *= lax.axis_size(name)
    return lax.ppermute(array, axis, [(i, (i + by) % count) for i in range(count)])


def after(value, *others):
    return lax.optimization_barrier((value,) + others)[0]


def gathered(array, axis, sign=1):
    held, by = array[None], 1
    while by < lax.axis_size(axis):
        held = jnp.concatenate([held, shifted(held, axis, sign * by)], axis=0)
        by *= 2
    return held


def thirds(x):
    pieces = []
    for _ in range(3):
        piece = lax.reduce_precision(x, 8, 7)
        pieces.append(piece.astype(BF16))
        x = x - piece
    return pieces


def ordered_hidden(expert_hidden, n_z, n_xc):
    experts, rows, _ = expert_hidden.shape
    half = n_z // 2
    used = half * CAP
    padded = n_xc * 2 * 32
    at = lax.broadcasted_iota(jnp.int32, (experts, padded, 1), 1)
    odd = lax.broadcasted_iota(jnp.int32, (experts, padded, 1), 0) % 2
    inner = at % 32 - odd * (32 - used)
    z = (lax.axis_index("z") + at // 32 % 2 * half + inner // CAP) % n_z
    xc = at // 64
    source = jnp.where((inner >= 0) & (inner < used), (z * n_xc + xc) * CAP + inner % CAP, -1)
    order = (source == lax.broadcasted_iota(jnp.int32, (1, 1, rows), 2)).astype(BF16)
    return jnp.einsum(
        "epr,erf->epf", order, expert_hidden, preferred_element_type=F32
    ).astype(BF16)


def produce_body(hidden_ref, weight_ref, out_ref):
    experts = hidden_ref.shape[0]
    made = [dot(hidden_ref[e], weight_ref[e]) for e in range(experts)]
    for group in range(out_ref.shape[0]):
        for half in range(2):
            at = (group * 2 + half) * 32
            pieces = []
            for e in range(0, experts, 2):
                a, b = made[e][at : at + 32], made[e + 1][at : at + 32]
                pieces += [a[:24], a[24:] + b[:8], b[8:]]
            rows = jnp.concatenate(pieces, axis=0)
            span = rows.shape[0]
            out_ref[group, half * span : (half + 1) * span, :] = rows.astype(BF16)


def produce(hidden, weight, start, cols, n_xc):
    experts, rows, units = hidden.shape
    block = 128
    while start % (2 * block) == 0 and cols % (2 * block) == 0 and block < 256:
        block *= 2
    sent = experts * 28 * 2
    return pl.pallas_call(
        produce_body,
        grid=(cols // block,),
        in_specs=[
            pl.BlockSpec((experts, rows, units), lambda n: (0, 0, 0)),
            pl.BlockSpec((experts, units, block), lambda n: (0, 0, start // block + n)),
        ],
        out_specs=pl.BlockSpec((n_xc, sent, block), lambda n: (0, 0, n)),
        out_shape=jax.ShapeDtypeStruct((n_xc, sent, cols), BF16),
        name="produce",
    )(hidden, weight)


def combine_matrix(tables, top, experts_of, n_xc):
    n_z, tokens, _ = tables.shape
    half = n_z // 2
    experts = experts_of * n_xc
    ids, weights = tables[..., :top], tables[..., top:]
    base = (lax.axis_index("z") * experts).astype(F32)
    named = ids[..., None] == base + jnp.arange(experts, dtype=F32)
    counts = jnp.sum(named.astype(F32), axis=2)
    dense = jnp.sum(jnp.where(named, weights[..., None], 0.0), axis=2).astype(BF16)
    earlier = (
        lax.broadcasted_iota(jnp.int32, (tokens, tokens), 0)
        > lax.broadcasted_iota(jnp.int32, (tokens, tokens), 1)
    ).astype(BF16)
    prior = jnp.einsum("tp,zpe->zte", earlier, counts.astype(BF16), preferred_element_type=F32)
    each = experts_of * half * CAP
    rows = each * n_xc
    at = lax.broadcasted_iota(jnp.int32, (experts, rows), 1)
    owner = at // (half * CAP)
    pick = (owner == lax.broadcasted_iota(jnp.int32, (experts, rows), 0)).astype(BF16)
    prior_rows = jnp.einsum("zte,er->ztr", prior.astype(BF16), pick, preferred_element_type=F32)
    dense_rows = jnp.einsum("zte,er->ztr", dense, pick, preferred_element_type=F32)
    at = lax.broadcasted_iota(jnp.int32, (n_z, 1, rows), 2)
    mine = at % (half * CAP) // CAP == lax.broadcasted_iota(jnp.int32, (n_z, 1, rows), 0) % half
    hit = mine & (prior_rows == (at % CAP).astype(F32))
    return jnp.where(hit, dense_rows, 0.0).astype(BF16).reshape(2, half * tokens, rows)


def combine_body(me_ref, combine_ref, got_ref, *outs):
    n_xc, rows, cols = got_ref.shape
    rows //= 2
    tokens = outs[0].shape[-2]
    half = combine_ref.shape[1] // tokens
    for h in range(2):
        filled = got_ref[:, h * rows : (h + 1) * rows, :].reshape(n_xc * rows, cols)
        sums = dot(combine_ref[h], filled)
        for z in range(half):
            rounded = sums[z * tokens : (z + 1) * tokens].astype(BF16)
            if len(outs) == 1:
                outs[0][lax.rem(me_ref[0] + h * half + z, 2 * half)] = rounded
            else:
                outs[h * half + z][...] = rounded


def combine_rows(combine, got, n_z, stacked):
    tokens = combine.shape[1] * 2 // n_z
    cols = got.shape[2]
    if stacked:
        outs = [jax.ShapeDtypeStruct((n_z, tokens, cols), BF16)]
    else:
        outs = [jax.ShapeDtypeStruct((tokens, cols), BF16)] * n_z
    return pl.pallas_call(
        combine_body,
        in_specs=[SCALARS, WHOLE, WHOLE],
        out_specs=[WHOLE] * len(outs),
        out_shape=outs,
        name="combine",
    )(lax.axis_index("z")[None], combine, got)


def sum_rounded(*parts):
    total = parts[0].astype(F32)
    for part in parts[1:]:
        total = total + part.astype(F32)
    return total.astype(BF16)


def sum_over_z(parts, upward):
    up = shifted(parts[3], "z", 1)
    down = shifted(parts[5], "z", -1)
    far = shifted(parts[4], "z", 2 if upward else -2)
    near = [shifted(parts[1], "z", 1), shifted(parts[7], "z", -1)]
    plus = sum_rounded(*([parts[2], up] + ([far] if upward else [])))
    minus = sum_rounded(*([parts[6], down] + ([] if upward else [far])))
    return [parts[0]] + near + [shifted(plus, "z", 2), shifted(minus, "z", -2)]


def maps_body(q_ref, k_ref, sum_col_ref, sum_row_ref, rate_col_ref, rate_row_ref, v_map_ref, s_map_ref):
    span = q_ref.shape[1]
    row = lax.broadcasted_iota(jnp.int32, (span, span), 0)
    col = lax.broadcasted_iota(jnp.int32, (span, span), 1)
    ident = (row == col).astype(F32)
    heads = v_map_ref.shape[1]
    share = heads // (q_ref.shape[2] // DK)
    every = range(heads)
    queries, keys, keys_t, met = [], [], [], []
    for at in range(0, q_ref.shape[2], DK):
        q = q_ref[0, :, at : at + DK].astype(F32)
        k = k_ref[0, :, at : at + DK].astype(F32)
        q = q * lax.rsqrt(jnp.sum(q * q, axis=-1, keepdims=True) + 1e-06) * DK ** (-0.5)
        k = k * lax.rsqrt(jnp.sum(k * k, axis=-1, keepdims=True) + 1e-06)
        queries.append(q)
        keys.append(k)
        keys_t.append(k.T)
        met.append(dot_split(jnp.concatenate([k, q], axis=0), keys_t[-1]))
    lower, scores, inverse = [], [], []
    for head in every:
        away = sum_col_ref[0, 0, :, head : head + 1] - sum_row_ref[0, 0, head : head + 1, :]
        ratio = jnp.where(row >= col, jnp.exp(jnp.where(row >= col, away, 0.0)), 0.0)
        pair = met[head // share]
        rate = rate_col_ref[0, 0, :, head : head + 1]
        lower.append(jnp.where(row > col, rate * ratio * pair[:span], 0.0))
        scores.append(ratio * pair[span:])
    small = [jnp.where(row // 8 == col // 8, lower[h], 0.0) for h in every]
    square = [dot_split(small[h], small[h]) for h in every]
    inverse = [dot_split(ident - small[h], ident + square[h]) for h in every]
    fourth = [dot_split(square[h], square[h]) for h in every]
    inverse = [dot_split(inverse[h], ident + fourth[h]) for h in every]
    size = 8
    while size < span:
        between = (row // (2 * size) == col // (2 * size)) & (row // size != col // size)
        moved = [dot_split(jnp.where(between, lower[h], 0.0), inverse[h]) for h in every]
        inverse = [inverse[h] - dot_split(inverse[h], moved[h]) for h in every]
        size *= 2
    v_maps = []
    for head in every:
        sum_row = sum_row_ref[0, 0, head : head + 1, :]
        tail = keys_t[head // share] * jnp.exp(sum_row[:, span - 1 : span] - sum_row)
        solve = inverse[head] * rate_row_ref[0, 0, head : head + 1, :]
        v_maps.append(dot_split(jnp.concatenate([scores[head], tail], axis=0), solve))
        v_map_ref[0, head] = jnp.concatenate(halves(v_maps[-1]), axis=1)
    for head in every:
        growth = jnp.exp(sum_col_ref[0, 0, :, head : head + 1])
        whole = jnp.exp(sum_row_ref[0, 0, head : head + 1, span - 1 : span])
        fixed = jnp.concatenate([growth * queries[head // share], whole * ident], axis=0)
        s_map = fixed - dot_split(v_maps[head], growth * keys[head // share])
        s_map_ref[0, head] = jnp.concatenate(halves(s_map), axis=1)


def key_maps(*args):
    blocks, span, _ = args[0].shape
    heads = args[3].shape[1] * args[3].shape[2]
    out = jax.ShapeDtypeStruct((blocks, heads, span + DK, 2 * span), BF16)

    groups = args[0].shape[2] // DK
    share = heads // groups
    field = pl.BlockSpec((1, span, DK), lambda n, g: (n, 0, g))
    columns = pl.BlockSpec((1, 1, span, share), lambda n, g: (n, g, 0, 0))
    rows = pl.BlockSpec((1, 1, share, span), lambda n, g: (n, g, 0, 0))
    made = pl.BlockSpec((1, share, span + DK, 2 * span), lambda n, g: (n, g, 0, 0))
    return pl.pallas_call(
        maps_body,
        grid=(blocks, groups),
        in_specs=[field, field, columns, rows, columns, rows],
        out_specs=[made, made],
        out_shape=[out, out],
        name="key_maps",
    )(*args)


def order_body(at_ref, own_ref, other_ref, out_ref):
    n_x, n_z, rows, _ = own_ref.shape
    n_c = 2
    for z in range(n_z):
        for x in range(n_x):
            for c in range(n_c):
                place = ((z * n_x + x) * n_c + c) * rows
                at = (lax.rem(at_ref[1] - x + n_x, n_x), lax.rem(at_ref[0] - z + n_z, n_z))
                here, there = own_ref[at], other_ref[at]
                out_ref[place : place + rows, :] = jnp.where(at_ref[2] == c, here, there)


def finish_body(n_sa, me_ref, gain_ref, weight_ref, v_map_ref, s_map_ref, *refs):
    streams, outs = refs[: -n_sa - 2], refs[-n_sa - 2 : -2]
    normed_ref, head_ref = refs[-2:]
    tokens, own = outs[0].shape
    heads = v_map_ref.shape[1]
    width = normed_ref.shape[1]
    me = me_ref[0]
    gain = gain_ref[...].astype(F32)
    for s in range(n_sa):
        stream = jnp.concatenate([a[...] for a in streams[s::n_sa]], axis=1).astype(F32)
        scale = lax.rsqrt(jnp.sum(stream * stream, axis=-1, keepdims=True) / width + 1e-06)
        normed_ref[s * tokens : (s + 1) * tokens, :] = (stream * scale * gain).astype(BF16)
    made = dot(normed_ref[...], weight_ref[...]).astype(BF16)
    for s in range(n_sa):
        head_ref[lax.rem(me - s + n_sa, n_sa)] = made[s * tokens : (s + 1) * tokens]
    states = [None] * heads
    for n in range(n_sa):
        at = lax.rem(me - n + n_sa, n_sa)
        for head in range(heads):
            lanes = slice(head * DV, (head + 1) * DV)
            v = head_ref[n, :, lanes]
            out = dot(v_map_ref[at, head], jnp.concatenate([v, v], axis=0))
            if n > 0:
                high, low = halves(states[head])
                maps = s_map_ref[at, head]
                out = out + dot(maps, jnp.concatenate([high, high], axis=0))
                out = out + dot(maps[:, :DK], low)
            head_ref[n, :, lanes] = out[:tokens].astype(BF16)
            states[head] = out[tokens:]
    for s in range(n_sa):
        outs[s][...] = head_ref[lax.rem(me + s, n_sa)]


def finish(me, gain, weight, v_map, s_map, streams, n_sa):
    tokens = streams[0].shape[0]
    width, own = weight.shape

    def body(*refs):
        finish_body(n_sa, *refs)

    return pl.pallas_call(
        body,
        in_specs=[SCALARS] + [WHOLE] * (4 + len(streams)),
        out_specs=[WHOLE] * n_sa,
        out_shape=[jax.ShapeDtypeStruct((tokens, own), BF16)] * n_sa,
        scratch_shapes=[
            pltpu.VMEM((n_sa * tokens, width), BF16),
            pltpu.VMEM((n_sa, tokens, own), BF16),
        ],
        name="finish",
    )(me, gain, weight, v_map, s_map, *streams)


def place_body(me_ref, *refs):
    got, out_ref = refs[:-1], refs[-1]
    own = got[0].shape[1]
    for s, ref in enumerate(got):
        at = lax.rem(me_ref[0] - s + len(got), len(got))
        out_ref[:, pl.ds(pl.multiple_of(at * own, own), own)] = ref[...]


def key_arguments(qk, extra, tokens):
    n_sa = qk.shape[0]
    heads = HV // n_sa
    rates = qk[:, tokens : tokens + extra].reshape(n_sa, 3, 2 * heads, tokens).astype(F32)
    rates = rates[:, 0] + rates[:, 1] + rates[:, 2]
    qk = qk[:, :tokens]
    until = (
        lax.broadcasted_iota(jnp.int32, (tokens, tokens), 0)
        <= lax.broadcasted_iota(jnp.int32, (tokens, tokens), 1)
    ).astype(F32)
    sum_row = jnp.einsum("nhp,pt->nht", rates[:, :heads], until, precision=HIGHEST)
    rate_row = rates[:, heads:]
    half = qk.shape[2] // 2
    by_key_head = (n_sa, half // DK, -1, tokens)
    sum_row, rate_row = sum_row.reshape(by_key_head), rate_row.reshape(by_key_head)
    return (
        qk[..., :half],
        qk[..., half:],
        sum_row.transpose(0, 1, 3, 2),
        sum_row,
        rate_row.transpose(0, 1, 3, 2),
        rate_row,
    )


def on_device(
    expert_hidden,
    down_weight,
    residual,
    expert_ids,
    combine_weight,
    norm_gain,
    value_weight,
    queries,
    keys,
    log_decay,
    write_rate,
):
    n_z, n_x, n_c, n_sa = (lax.axis_size(a) for a in ("z", "x", "c", "sa"))
    n_xc = n_x * n_c
    exp_dev, _, width = down_weight.shape
    tokens = residual.shape[1]
    top = expert_ids.shape[2]
    own = width // n_sa
    heads = HV // n_sa
    sa = lax.axis_index("sa")
    me = sa[None]

    hidden = ordered_hidden(expert_hidden, n_z, n_xc)
    made = produce(hidden, down_weight, 0, CHUNKS[0], n_xc)

    table = jnp.concatenate([expert_ids[0].astype(F32), combine_weight[0]], axis=1).T
    tables = gathered(after(table, made), "z", -1)
    combine = combine_matrix(tables.transpose(0, 2, 1), top, exp_dev, n_xc)

    part = lax.dynamic_slice_in_dim(value_weight, sa * own, own, axis=1)
    part = gathered(after(part, combine), "z")

    def by_group(array):
        return array[0].reshape(tokens, n_sa, -1).transpose(1, 0, 2)

    log_decay, write_rate, queries, keys = lax.optimization_barrier(
        (log_decay, write_rate, queries, keys, made)
    )[:4]
    rates = jnp.concatenate(
        [log_decay[0].T.reshape(n_sa, heads, tokens), write_rate[0].T.reshape(n_sa, heads, tokens)],
        axis=1,
    )
    rates = jnp.stack(thirds(rates), axis=1).reshape(n_sa, -1, own)
    extra = rates.shape[1]
    rates = jnp.pad(rates, ((0, 0), (0, -extra % 8), (0, 0)))
    sent = jnp.concatenate([by_group(queries), by_group(keys)], axis=2)
    sent = jnp.concatenate([sent, rates], axis=1)
    qk = []
    for s in range(n_sa):
        piece = lax.dynamic_index_in_dim(sent, (sa + s) % n_sa, keepdims=False)
        qk.append(shifted(piece, "sa", s) if s else piece)
    qk = jnp.stack(qk)

    start = 0
    streams = []
    for number, cols in enumerate(CHUNKS):
        final = number == len(CHUNKS) - 1
        got = lax.all_to_all(made, ("x", "c"), split_axis=0, concat_axis=0, tiled=True)
        if final:
            part = after(part, got)
            part = jnp.stack([part] + [shifted(part, "x", r) for r in range(1, n_x)])
        if not final:
            gate = parts if number else (combine,)
            made = produce(after(hidden, *gate), down_weight, start + cols, CHUNKS[number + 1], n_xc)
            if number:
                made = after(made, got, part)
            else:
                made, qk = lax.optimization_barrier((made, qk, got))[:2]
        weighting = after(combine, *parts) if final else combine
        parts = combine_rows(weighting, got, n_z, final)
        if final:
            v_map, s_map = key_maps(*key_arguments(after(qk, *parts), extra, tokens))
            parts = lax.all_to_all(parts[0], "z", split_axis=0, concat_axis=0, tiled=True)
            parts = after(parts, v_map)
            parts = [parts[z] for z in range(n_z)]
        else:
            parts = sum_over_z(parts, number % 2 == 0)
        stream = sum_rounded(residual[0, :, start : start + cols], *parts)
        streams += [stream] + [shifted(stream, "sa", s) for s in range(1, n_sa)]
        start += cols
    place = jnp.stack([lax.axis_index(a) for a in ("z", "x", "c")])
    projection = pl.pallas_call(
        order_body,
        in_specs=[SCALARS, WHOLE, WHOLE],
        out_specs=WHOLE,
        out_shape=jax.ShapeDtypeStruct((width, own), BF16),
        name="order",
    )(place, part, shifted(part, "c", 1))
    outs = finish(me, norm_gain[None], projection, v_map, s_map, streams, n_sa)
    outs = [outs[0]] + [shifted(outs[s], "sa", s) for s in range(1, n_sa)]
    out = pl.pallas_call(
        place_body,
        in_specs=[SCALARS] + [WHOLE] * n_sa,
        out_specs=WHOLE,
        out_shape=jax.ShapeDtypeStruct((tokens, width), BF16),
        name="place",
    )(me, *outs)
    return out[None]


def solution(mesh):
    fine = Mesh(mesh.devices.reshape(8, 4, 2, 4), ("z", "x", "c", "sa"))
    ea = ("z", "x", "c")
    return jax.shard_map(
        on_device,
        mesh=fine,
        in_specs=(
            P(ea, "sa", None),
            P(ea, None, None),
            P(ea, "sa", None),
            P(ea, "sa", None),
            P(ea, "sa", None),
            P(),
            P(ea, None),
            P(ea, "sa", None),
            P(ea, "sa", None),
            P(ea, "sa", None),
            P(ea, "sa", None),
        ),
        out_specs=P(ea, "sa", None),
        check_vma=False,
    )
```

```python
import jax
import jax.numpy as jnp
from jax import lax
from jax.experimental import pallas as pl
from jax.experimental.pallas import tpu as pltpu
from jax.sharding import Mesh, PartitionSpec as P


HV = 16
DK = 128
DV = 128
CAP = 7
CHUNKS = (768, 768, 512)
HIGHEST = lax.Precision.HIGHEST
F32 = jnp.float32
BF16 = jnp.bfloat16
WHOLE = pl.BlockSpec(memory_space=pltpu.VMEM)
SCALARS = pl.BlockSpec(memory_space=pltpu.SMEM)


def dot(a, b):
    return jnp.dot(a, b, preferred_element_type=F32)


def halves(x):
    high = x.astype(BF16)
    return high, (x - high.astype(F32)).astype(BF16)


def dot_split(a, b):
    a_high, a_low = halves(a)
    b_high, b_low = halves(b)
    both = jnp.concatenate([a_high, a_low], axis=1)
    return dot(both, jnp.concatenate([b_high, b_high], axis=0)) + dot(a_high, b_low)


def shifted(array, axis, by):
    names = axis if isinstance(axis, tuple) else (axis,)
    count = 1
    for name in names:
        count *= lax.axis_size(name)
    return lax.ppermute(array, axis, [(i, (i + by) % count) for i in range(count)])


def after(value, *others):
    return lax.optimization_barrier((value,) + others)[0]


def gathered(array, axis, sign=1):
    held, by = array[None], 1
    while by < lax.axis_size(axis):
        moved = shifted(held, axis, sign * by)
        held = jnp.concatenate([held, moved], axis=0)
        by *= 2
    return held


def thirds(x):
    pieces = []
    for _ in range(3):
        piece = lax.reduce_precision(x, 8, 7)
        pieces.append(piece.astype(BF16))
        x = x - piece
    return pieces


def ordered_hidden(expert_hidden, n_z, n_xc):
    experts, rows, _ = expert_hidden.shape
    half = n_z // 2
    used = half * CAP
    padded = n_xc * 2 * 32
    at = lax.broadcasted_iota(jnp.int32, (experts, padded, 1), 1)
    odd = lax.broadcasted_iota(jnp.int32, (experts, padded, 1), 0) % 2
    inner = at % 32 - odd * (32 - used)
    z = (lax.axis_index("z") + at // 32 % 2 * half + inner // CAP) % n_z
    xc = at // 64
    source = jnp.where((inner >= 0) & (inner < used), (z * n_xc + xc) * CAP + inner % CAP, -1)
    order = (source == lax.broadcasted_iota(jnp.int32, (1, 1, rows), 2)).astype(BF16)
    return jnp.einsum(
        "epr,erf->epf", order, expert_hidden, preferred_element_type=F32
    ).astype(BF16)


def produce_body(hidden_ref, weight_ref, out_ref):
    experts = hidden_ref.shape[0]
    made = [dot(hidden_ref[e], weight_ref[e]) for e in range(experts)]
    for group in range(out_ref.shape[0]):
        for half in range(2):
            at = (group * 2 + half) * 32
            pieces = []
            for e in range(0, experts, 2):
                a, b = made[e][at : at + 32], made[e + 1][at : at + 32]
                pieces += [a[:24], a[24:] + b[:8], b[8:]]
            rows = jnp.concatenate(pieces, axis=0)
            span = rows.shape[0]
            out_ref[group, half * span : (half + 1) * span, :] = rows.astype(BF16)


def produce(hidden, weight, start, cols, n_xc):
    experts, rows, units = hidden.shape
    block = 128
    while start % (2 * block) == 0 and cols % (2 * block) == 0 and block < 256:
        block *= 2
    sent = experts * 28 * 2
    return pl.pallas_call(
        produce_body,
        grid=(cols // block,),
        in_specs=[
            pl.BlockSpec((experts, rows, units), lambda n: (0, 0, 0)),
            pl.BlockSpec((experts, units, block), lambda n: (0, 0, start // block + n)),
        ],
        out_specs=pl.BlockSpec((n_xc, sent, block), lambda n: (0, 0, n)),
        out_shape=jax.ShapeDtypeStruct((n_xc, sent, cols), BF16),
        name="produce",
    )(hidden, weight)


def combine_matrix(tables, top, experts_of, n_xc):
    n_z, tokens, _ = tables.shape
    half = n_z // 2
    experts = experts_of * n_xc
    ids, weights = tables[..., :top], tables[..., top:]
    base = (lax.axis_index("z") * experts).astype(F32)
    named = ids[..., None] == base + jnp.arange(experts, dtype=F32)
    counts = jnp.sum(named.astype(F32), axis=2)
    dense = jnp.sum(jnp.where(named, weights[..., None], 0.0), axis=2).astype(BF16)
    earlier = (
        lax.broadcasted_iota(jnp.int32, (tokens, tokens), 0)
        > lax.broadcasted_iota(jnp.int32, (tokens, tokens), 1)
    ).astype(BF16)
    prior = jnp.einsum("tp,zpe->zte", earlier, counts.astype(BF16), preferred_element_type=F32)
    each = experts_of * half * CAP
    rows = each * n_xc
    at = lax.broadcasted_iota(jnp.int32, (experts, rows), 1)
    owner = at // (half * CAP)
    pick = (owner == lax.broadcasted_iota(jnp.int32, (experts, rows), 0)).astype(BF16)
    prior_rows = jnp.einsum("zte,er->ztr", prior.astype(BF16), pick, preferred_element_type=F32)
    dense_rows = jnp.einsum("zte,er->ztr", dense, pick, preferred_element_type=F32)
    at = lax.broadcasted_iota(jnp.int32, (n_z, 1, rows), 2)
    mine = at % (half * CAP) // CAP == lax.broadcasted_iota(jnp.int32, (n_z, 1, rows), 0) % half
    hit = mine & (prior_rows == (at % CAP).astype(F32))
    return jnp.where(hit, dense_rows, 0.0).astype(BF16).reshape(2, half * tokens, rows)


def combine_body(me_ref, combine_ref, got_ref, *outs):
    n_xc, rows, cols = got_ref.shape
    rows //= 2
    tokens = outs[0].shape[-2]
    half = combine_ref.shape[1] // tokens
    for h in range(2):
        filled = got_ref[:, h * rows : (h + 1) * rows, :].reshape(n_xc * rows, cols)
        sums = dot(combine_ref[h], filled)
        for z in range(half):
            rounded = sums[z * tokens : (z + 1) * tokens].astype(BF16)
            if len(outs) == 1:
                outs[0][lax.rem(me_ref[0] + h * half + z, 2 * half)] = rounded
            else:
                outs[h * half + z][...] = rounded


def combine_rows(combine, got, n_z, stacked):
    tokens = combine.shape[1] * 2 // n_z
    cols = got.shape[2]
    block = 256
    if stacked:
        outs = [jax.ShapeDtypeStruct((n_z, tokens, cols), BF16)]
        specs = [pl.BlockSpec((n_z, tokens, block), lambda n: (0, 0, n))]
    else:
        outs = [jax.ShapeDtypeStruct((tokens, cols), BF16)] * n_z
        specs = [pl.BlockSpec((tokens, block), lambda n: (0, n))] * n_z
    return pl.pallas_call(
        combine_body,
        grid=(cols // block,),
        in_specs=[
            SCALARS,
            pl.BlockSpec(combine.shape, lambda n: (0, 0, 0)),
            pl.BlockSpec(got.shape[:2] + (block,), lambda n: (0, 0, n)),
        ],
        out_specs=specs,
        out_shape=outs,
        name="combine",
    )(lax.axis_index("z")[None], combine, got)


def sum_rounded(*parts):
    total = parts[0].astype(F32)
    for part in parts[1:]:
        total = total + part.astype(F32)
    return total.astype(BF16)


def start_sum_over_z(parts, upward):
    up = shifted(parts[3], "z", 1)
    down = shifted(parts[5], "z", -1)
    far = shifted(parts[4], "z", 2 if upward else -2)
    plus = [parts[2], up] + ([far] if upward else [])
    minus = [parts[6], down] + ([] if upward else [far])
    near = [shifted(parts[1], "z", 1), shifted(parts[7], "z", -1)]
    return plus, minus, [parts[0]] + near


def pass_on(plus, minus, near, gate):
    *plus, _ = lax.optimization_barrier((*plus, gate))
    *minus, _ = lax.optimization_barrier((*minus, gate))
    sums = [sum_rounded(*plus), sum_rounded(*minus)]
    return sums, near + [shifted(sums[0], "z", 2), shifted(sums[1], "z", -2)]


def maps_body(q_ref, k_ref, sum_col_ref, sum_row_ref, rate_col_ref, rate_row_ref, v_map_ref, s_map_ref):
    span = q_ref.shape[1]
    row = lax.broadcasted_iota(jnp.int32, (span, span), 0)
    col = lax.broadcasted_iota(jnp.int32, (span, span), 1)
    ident = (row == col).astype(F32)
    heads = v_map_ref.shape[1]
    share = heads // (q_ref.shape[2] // DK)
    every = range(heads)
    queries, keys, keys_t, met = [], [], [], []
    for at in range(0, q_ref.shape[2], DK):
        q = q_ref[0, :, at : at + DK].astype(F32)
        k = k_ref[0, :, at : at + DK].astype(F32)
        q = q * lax.rsqrt(jnp.sum(q * q, axis=-1, keepdims=True) + 1e-06) * DK ** (-0.5)
        k = k * lax.rsqrt(jnp.sum(k * k, axis=-1, keepdims=True) + 1e-06)
        queries.append(q)
        keys.append(k)
        keys_t.append(k.T)
        met.append(dot_split(jnp.concatenate([k, q], axis=0), keys_t[-1]))
    lower, scores, inverse = [], [], []
    for head in every:
        away = sum_col_ref[0, :, head : head + 1] - sum_row_ref[0, head : head + 1, :]
        ratio = jnp.where(row >= col, jnp.exp(jnp.where(row >= col, away, 0.0)), 0.0)
        pair = met[head // share]
        rate = rate_col_ref[0, :, head : head + 1]
        lower.append(jnp.where(row > col, rate * ratio * pair[:span], 0.0))
        scores.append(ratio * pair[span:])
    small = [jnp.where(row // 8 == col // 8, lower[h], 0.0) for h in every]
    square = [dot_split(small[h], small[h]) for h in every]
    inverse = [dot_split(ident - small[h], ident + square[h]) for h in every]
    fourth = [dot_split(square[h], square[h]) for h in every]
    inverse = [dot_split(inverse[h], ident + fourth[h]) for h in every]
    size = 8
    while size < span:
        between = (row // (2 * size) == col // (2 * size)) & (row // size != col // size)
        moved = [dot_split(jnp.where(between, lower[h], 0.0), inverse[h]) for h in every]
        inverse = [inverse[h] - dot_split(inverse[h], moved[h]) for h in every]
        size *= 2
    v_maps = []
    for head in every:
        sum_row = sum_row_ref[0, head : head + 1, :]
        tail = keys_t[head // share] * jnp.exp(sum_row[:, span - 1 : span] - sum_row)
        solve = inverse[head] * rate_row_ref[0, head : head + 1, :]
        v_maps.append(dot_split(jnp.concatenate([scores[head], tail], axis=0), solve))
        v_map_ref[0, head] = jnp.concatenate(halves(v_maps[-1]), axis=1)
    for head in every:
        growth = jnp.exp(sum_col_ref[0, :, head : head + 1])
        whole = jnp.exp(sum_row_ref[0, head : head + 1, span - 1 : span])
        fixed = jnp.concatenate([growth * queries[head // share], whole * ident], axis=0)
        s_map = fixed - dot_split(v_maps[head], growth * keys[head // share])
        s_map_ref[0, head] = jnp.concatenate(halves(s_map), axis=1)


def key_maps(*args):
    blocks, span, _ = args[0].shape
    heads = args[3].shape[1]
    out = jax.ShapeDtypeStruct((blocks, heads, span + DK, 2 * span), BF16)

    def whole(array):
        return pl.BlockSpec((1,) + array.shape[1:], lambda n: (n,) + (0,) * (array.ndim - 1))

    return pl.pallas_call(
        maps_body,
        grid=(blocks,),
        in_specs=[whole(a) for a in args],
        out_specs=[whole(out), whole(out)],
        out_shape=[out, out],
        name="key_maps",
    )(*args)


def order_body(at_ref, own_ref, other_ref, out_ref):
    n_x, n_z, rows, _ = own_ref.shape
    n_c = 2
    for z in range(n_z):
        for x in range(n_x):
            for c in range(n_c):
                place = ((z * n_x + x) * n_c + c) * rows
                at = (lax.rem(at_ref[1] - x + n_x, n_x), lax.rem(at_ref[0] - z + n_z, n_z))
                here, there = own_ref[at], other_ref[at]
                out_ref[place : place + rows, :] = jnp.where(at_ref[2] == c, here, there)


def finish_body(n_sa, me_ref, gain_ref, weight_ref, v_map_ref, s_map_ref, *refs):
    streams, outs = refs[: -n_sa - 2], refs[-n_sa - 2 : -2]
    normed_ref, head_ref = refs[-2:]
    tokens, own = outs[0].shape
    heads = v_map_ref.shape[1]
    width = normed_ref.shape[1]
    me = me_ref[0]
    gain = gain_ref[...].astype(F32)
    for s in range(n_sa):
        stream = jnp.concatenate([a[...] for a in streams[s::n_sa]], axis=1).astype(F32)
        scale = lax.rsqrt(jnp.sum(stream * stream, axis=-1, keepdims=True) / width + 1e-06)
        normed_ref[s * tokens : (s + 1) * tokens, :] = (stream * scale * gain).astype(BF16)

    @pl.loop(0, own, step=256)
    def _(at):
        lanes = pl.ds(pl.multiple_of(at, 256), 256)
        made = dot(normed_ref[...], weight_ref[:, lanes]).astype(BF16)
        for s in range(n_sa):
            head_ref[lax.rem(me - s + n_sa, n_sa), :, lanes] = made[s * tokens : (s + 1) * tokens]

    states = [None] * heads
    for n in range(n_sa):
        at = lax.rem(me - n + n_sa, n_sa)
        for head in range(heads):
            lanes = slice(head * DV, (head + 1) * DV)
            v = head_ref[n, :, lanes]
            out = dot(v_map_ref[at, head], jnp.concatenate([v, v], axis=0))
            if n > 0:
                high, low = halves(states[head])
                maps = s_map_ref[at, head]
                out = out + dot(maps, jnp.concatenate([high, high], axis=0))
                out = out + dot(maps[:, :DK], low)
            head_ref[n, :, lanes] = out[:tokens].astype(BF16)
            states[head] = out[tokens:]
    for s in range(n_sa):
        outs[s][...] = head_ref[lax.rem(me + s, n_sa)]


def finish(me, gain, weight, v_map, s_map, streams, n_sa):
    tokens = streams[0].shape[0]
    width, own = weight.shape

    def body(*refs):
        finish_body(n_sa, *refs)

    return pl.pallas_call(
        body,
        in_specs=[SCALARS] + [WHOLE] * (4 + len(streams)),
        out_specs=[WHOLE] * n_sa,
        out_shape=[jax.ShapeDtypeStruct((tokens, own), BF16)] * n_sa,
        scratch_shapes=[
            pltpu.VMEM((n_sa * tokens, width), BF16),
            pltpu.VMEM((n_sa, tokens, own), BF16),
        ],
        name="finish",
    )(me, gain, weight, v_map, s_map, *streams)


def place_body(me_ref, *refs):
    got, out_ref = refs[:-1], refs[-1]
    own = got[0].shape[1]
    for s, ref in enumerate(got):
        at = lax.rem(me_ref[0] - s + len(got), len(got))
        out_ref[:, pl.ds(pl.multiple_of(at * own, own), own)] = ref[...]


def key_arguments(qk, extra, tokens):
    n_sa = qk.shape[0]
    heads = HV // n_sa
    rates = qk[:, tokens : tokens + extra].reshape(n_sa, 3, 2 * heads, tokens).astype(F32)
    rates = rates[:, 0] + rates[:, 1] + rates[:, 2]
    qk = qk[:, :tokens]
    until = (
        lax.broadcasted_iota(jnp.int32, (tokens, tokens), 0)
        <= lax.broadcasted_iota(jnp.int32, (tokens, tokens), 1)
    ).astype(F32)
    sum_row = jnp.einsum("nhp,pt->nht", rates[:, :heads], until, precision=HIGHEST)
    rate_row = rates[:, heads:]
    half = qk.shape[2] // 2
    return (
        qk[..., :half],
        qk[..., half:],
        sum_row.transpose(0, 2, 1),
        sum_row,
        rate_row.transpose(0, 2, 1),
        rate_row,
    )


def on_device(
    expert_hidden,
    down_weight,
    residual,
    expert_ids,
    combine_weight,
    norm_gain,
    value_weight,
    queries,
    keys,
    log_decay,
    write_rate,
):
    n_z, n_x, n_c, n_sa = (lax.axis_size(a) for a in ("z", "x", "c", "sa"))
    n_xc = n_x * n_c
    exp_dev, _, width = down_weight.shape
    tokens = residual.shape[1]
    top = expert_ids.shape[2]
    own = width // n_sa
    heads = HV // n_sa
    sa = lax.axis_index("sa")
    me = sa[None]

    hidden = ordered_hidden(expert_hidden, n_z, n_xc)
    made = produce(hidden, down_weight, 0, CHUNKS[0], n_xc)

    table = jnp.concatenate([expert_ids[0].astype(F32), combine_weight[0]], axis=1).T
    tables = gathered(after(table, made), "z", -1)
    combine = combine_matrix(tables.transpose(0, 2, 1), top, exp_dev, n_xc)

    part = lax.dynamic_slice_in_dim(value_weight, sa * own, own, axis=1)
    part = gathered(after(part, combine), "z")

    def by_group(array):
        return array[0].reshape(tokens, n_sa, -1).transpose(1, 0, 2)

    log_decay, write_rate, queries, keys = lax.optimization_barrier(
        (log_decay, write_rate, queries, keys, made)
    )[:4]
    rates = jnp.concatenate(
        [log_decay[0].T.reshape(n_sa, heads, tokens), write_rate[0].T.reshape(n_sa, heads, tokens)],
        axis=1,
    )
    rates = jnp.stack(thirds(rates), axis=1).reshape(n_sa, -1, own)
    extra = rates.shape[1]
    rates = jnp.pad(rates, ((0, 0), (0, -extra % 8), (0, 0)))
    sent = jnp.concatenate([by_group(queries), by_group(keys)], axis=2)
    sent = jnp.concatenate([sent, rates], axis=1)
    qk = []
    for s in range(n_sa):
        piece = lax.dynamic_index_in_dim(sent, (sa + s) % n_sa, keepdims=False)
        qk.append(shifted(piece, "sa", s) if s else piece)
    qk = jnp.stack(qk)

    starts = [sum(CHUNKS[:n]) for n in range(len(CHUNKS))]

    def spread_stream(number, parts):
        own_part = residual[0, :, starts[number] : starts[number] + CHUNKS[number]]
        stream = sum_rounded(own_part, *parts)
        return [stream] + [shifted(stream, "sa", s) for s in range(1, n_sa)]

    def exchange(rows):
        return lax.all_to_all(rows, ("x", "c"), split_axis=0, concat_axis=0, tiled=True)

    def make(rows, number):
        return produce(rows, down_weight, starts[number], CHUNKS[number], n_xc)

    def gather_chunk(number, weighting, rows):
        return combine_rows(weighting, rows, n_z, number == 2)

    got = exchange(made)
    made = make(hidden, 1)
    made, qk, combine, got = lax.optimization_barrier((made, qk, combine, got))

    arrived = exchange(made)
    parts = gather_chunk(0, combine, got)
    first = start_sum_over_z(parts, True)
    made = make(after(hidden, parts[0]), 2)
    _, earlier = pass_on(*first, made)
    made, got = lax.optimization_barrier((made, arrived))

    arrived = exchange(made)
    parts = gather_chunk(1, combine, got)
    first = start_sum_over_z(parts, False)
    *earlier, _ = lax.optimization_barrier((*earlier, parts[0]))
    streams = spread_stream(0, earlier)
    sums, earlier = pass_on(*first, streams[0])
    combine, *_ = lax.optimization_barrier((combine, *sums))

    part = after(part, arrived)
    part = jnp.stack([part] + [shifted(part, "x", r) for r in range(1, n_x)])
    (parts,) = gather_chunk(2, combine, arrived)
    *earlier, _ = lax.optimization_barrier((*earlier, parts))
    streams += spread_stream(1, earlier)
    v_map, s_map = key_maps(*key_arguments(after(qk, parts), extra, tokens))
    parts = lax.all_to_all(parts, "z", split_axis=0, concat_axis=0, tiled=True)
    parts, v_map, s_map = lax.optimization_barrier((parts, v_map, s_map))
    streams += spread_stream(2, [parts[z] for z in range(n_z)])
    place = jnp.stack([lax.axis_index(a) for a in ("z", "x", "c")])
    projection = pl.pallas_call(
        order_body,
        in_specs=[SCALARS, WHOLE, WHOLE],
        out_specs=WHOLE,
        out_shape=jax.ShapeDtypeStruct((width, own), BF16),
        name="order",
    )(place, part, shifted(part, "c", 1))
    outs = finish(me, norm_gain[None], projection, v_map, s_map, streams, n_sa)
    outs = [outs[0]] + [shifted(outs[s], "sa", s) for s in range(1, n_sa)]
    out = pl.pallas_call(
        place_body,
        in_specs=[SCALARS] + [WHOLE] * n_sa,
        out_specs=WHOLE,
        out_shape=jax.ShapeDtypeStruct((tokens, width), BF16),
        name="place",
    )(me, *outs)
    return out[None]


def solution(mesh):
    fine = Mesh(mesh.devices.reshape(8, 4, 2, 4), ("z", "x", "c", "sa"))
    ea = ("z", "x", "c")
    return jax.shard_map(
        on_device,
        mesh=fine,
        in_specs=(
            P(ea, "sa", None),
            P(ea, None, None),
            P(ea, "sa", None),
            P(ea, "sa", None),
            P(ea, "sa", None),
            P(),
            P(ea, None),
            P(ea, "sa", None),
            P(ea, "sa", None),
            P(ea, "sa", None),
            P(ea, "sa", None),
        ),
        out_specs=P(ea, "sa", None),
        check_vma=False,
    )
```

```python
import jax
import jax.numpy as jnp
from jax import lax
from jax.experimental import pallas as pl
from jax.experimental.pallas import tpu as pltpu
from jax.sharding import Mesh, PartitionSpec as P


HV = 16
DK = 128
DV = 128
CAP = 7
CHUNKS = (768, 768, 512)
HIGHEST = lax.Precision.HIGHEST
F32 = jnp.float32
BF16 = jnp.bfloat16
WHOLE = pl.BlockSpec(memory_space=pltpu.VMEM)
SCALARS = pl.BlockSpec(memory_space=pltpu.SMEM)


def dot(a, b):
    return jnp.dot(a, b, preferred_element_type=F32)


def halves(x):
    high = x.astype(BF16)
    return high, (x - high.astype(F32)).astype(BF16)


def dot_split(a, b):
    a_high, a_low = halves(a)
    b_high, b_low = halves(b)
    both = jnp.concatenate([a_high, a_low], axis=1)
    return dot(both, jnp.concatenate([b_high, b_high], axis=0)) + dot(a_high, b_low)


def shifted(array, axis, by):
    names = axis if isinstance(axis, tuple) else (axis,)
    count = 1
    for name in names:
        count *= lax.axis_size(name)
    return lax.ppermute(array, axis, [(i, (i + by) % count) for i in range(count)])


def after(value, *others):
    return lax.optimization_barrier((value,) + others)[0]


def gathered(array, axis, sign=1):
    held, by = array[None], 1
    while by < lax.axis_size(axis):
        moved = shifted(held, axis, sign * by)
        held = jnp.concatenate([held, moved], axis=0)
        by *= 2
    return held


def thirds(x):
    pieces = []
    for _ in range(3):
        piece = lax.reduce_precision(x, 8, 7)
        pieces.append(piece.astype(BF16))
        x = x - piece
    return pieces


def ordered_hidden(expert_hidden, n_z, n_xc):
    experts, rows, _ = expert_hidden.shape
    half = n_z // 2
    used = half * CAP
    padded = n_xc * 2 * 32
    at = lax.broadcasted_iota(jnp.int32, (experts, padded, 1), 1)
    odd = lax.broadcasted_iota(jnp.int32, (experts, padded, 1), 0) % 2
    inner = at % 32 - odd * (32 - used)
    z = (lax.axis_index("z") + at // 32 % 2 * half + inner // CAP) % n_z
    xc = at // 64
    source = jnp.where((inner >= 0) & (inner < used), (z * n_xc + xc) * CAP + inner % CAP, -1)
    order = (source == lax.broadcasted_iota(jnp.int32, (1, 1, rows), 2)).astype(BF16)
    return jnp.einsum(
        "epr,erf->epf", order, expert_hidden, preferred_element_type=F32
    ).astype(BF16)


def produce_body(hidden_ref, weight_ref, out_ref):
    experts = hidden_ref.shape[0]
    made = [dot(hidden_ref[e], weight_ref[e]) for e in range(experts)]
    for group in range(out_ref.shape[0]):
        for half in range(2):
            at = (group * 2 + half) * 32
            pieces = []
            for e in range(0, experts, 2):
                a, b = made[e][at : at + 32], made[e + 1][at : at + 32]
                pieces += [a[:24], a[24:] + b[:8], b[8:]]
            rows = jnp.concatenate(pieces, axis=0)
            span = rows.shape[0]
            out_ref[group, half * span : (half + 1) * span, :] = rows.astype(BF16)


def produce(hidden, weight, start, cols, n_xc):
    experts, rows, units = hidden.shape
    block = 128
    while start % (2 * block) == 0 and cols % (2 * block) == 0 and block < 256:
        block *= 2
    sent = experts * 28 * 2
    return pl.pallas_call(
        produce_body,
        grid=(cols // block,),
        in_specs=[
            pl.BlockSpec((experts, rows, units), lambda n: (0, 0, 0)),
            pl.BlockSpec((experts, units, block), lambda n: (0, 0, start // block + n)),
        ],
        out_specs=pl.BlockSpec((n_xc, sent, block), lambda n: (0, 0, n)),
        out_shape=jax.ShapeDtypeStruct((n_xc, sent, cols), BF16),
        name="produce",
    )(hidden, weight)


def combine_matrix(tables, top, experts_of, n_xc):
    n_z, tokens, _ = tables.shape
    half = n_z // 2
    experts = experts_of * n_xc
    ids, weights = tables[..., :top], tables[..., top:]
    base = (lax.axis_index("z") * experts).astype(F32)
    named = ids[..., None] == base + jnp.arange(experts, dtype=F32)
    counts = jnp.sum(named.astype(F32), axis=2)
    dense = jnp.sum(jnp.where(named, weights[..., None], 0.0), axis=2).astype(BF16)
    earlier = (
        lax.broadcasted_iota(jnp.int32, (tokens, tokens), 0)
        > lax.broadcasted_iota(jnp.int32, (tokens, tokens), 1)
    ).astype(BF16)
    prior = jnp.einsum("tp,zpe->zte", earlier, counts.astype(BF16), preferred_element_type=F32)
    each = experts_of * half * CAP
    rows = each * n_xc
    at = lax.broadcasted_iota(jnp.int32, (experts, rows), 1)
    owner = at // (half * CAP)
    pick = (owner == lax.broadcasted_iota(jnp.int32, (experts, rows), 0)).astype(BF16)
    prior_rows = jnp.einsum("zte,er->ztr", prior.astype(BF16), pick, preferred_element_type=F32)
    dense_rows = jnp.einsum("zte,er->ztr", dense, pick, preferred_element_type=F32)
    at = lax.broadcasted_iota(jnp.int32, (n_z, 1, rows), 2)
    mine = at % (half * CAP) // CAP == lax.broadcasted_iota(jnp.int32, (n_z, 1, rows), 0) % half
    hit = mine & (prior_rows == (at % CAP).astype(F32))
    return jnp.where(hit, dense_rows, 0.0).astype(BF16).reshape(2, half * tokens, rows)


def combine_body(me_ref, combine_ref, got_ref, *outs):
    n_xc, rows, cols = got_ref.shape
    rows //= 2
    tokens = outs[0].shape[-2]
    half = combine_ref.shape[1] // tokens
    for h in range(2):
        filled = got_ref[:, h * rows : (h + 1) * rows, :].reshape(n_xc * rows, cols)
        sums = dot(combine_ref[h], filled)
        for z in range(half):
            rounded = sums[z * tokens : (z + 1) * tokens].astype(BF16)
            if len(outs) == 1:
                outs[0][lax.rem(me_ref[0] + h * half + z, 2 * half)] = rounded
            else:
                outs[h * half + z][...] = rounded


def combine_rows(combine, got, n_z, stacked):
    tokens = combine.shape[1] * 2 // n_z
    cols = got.shape[2]
    block = 256
    if stacked:
        outs = [jax.ShapeDtypeStruct((n_z, tokens, cols), BF16)]
        specs = [pl.BlockSpec((n_z, tokens, block), lambda n: (0, 0, n))]
    else:
        outs = [jax.ShapeDtypeStruct((tokens, cols), BF16)] * n_z
        specs = [pl.BlockSpec((tokens, block), lambda n: (0, n))] * n_z
    return pl.pallas_call(
        combine_body,
        grid=(cols // block,),
        in_specs=[
            SCALARS,
            pl.BlockSpec(combine.shape, lambda n: (0, 0, 0)),
            pl.BlockSpec(got.shape[:2] + (block,), lambda n: (0, 0, n)),
        ],
        out_specs=specs,
        out_shape=outs,
        name="combine",
    )(lax.axis_index("z")[None], combine, got)


def sum_rounded(*parts):
    total = parts[0].astype(F32)
    for part in parts[1:]:
        total = total + part.astype(F32)
    return total.astype(BF16)


def start_sum_over_z(parts, upward):
    up = shifted(parts[3], "z", 1)
    down = shifted(parts[5], "z", -1)
    far = shifted(parts[4], "z", 2 if upward else -2)
    plus = [parts[2], up] + ([far] if upward else [])
    minus = [parts[6], down] + ([] if upward else [far])
    near = [shifted(parts[1], "z", 1), shifted(parts[7], "z", -1)]
    return plus, minus, [parts[0]] + near


def pass_on(plus, minus, near, gate):
    *plus, _ = lax.optimization_barrier((*plus, gate))
    *minus, _ = lax.optimization_barrier((*minus, gate))
    sums = [sum_rounded(*plus), sum_rounded(*minus)]
    return sums, near + [shifted(sums[0], "z", 2), shifted(sums[1], "z", -2)]


def maps_body(q_ref, k_ref, sum_col_ref, sum_row_ref, rate_col_ref, rate_row_ref, v_map_ref, s_map_ref):
    span = q_ref.shape[1]
    row = lax.broadcasted_iota(jnp.int32, (span, span), 0)
    col = lax.broadcasted_iota(jnp.int32, (span, span), 1)
    ident = (row == col).astype(F32)
    heads = v_map_ref.shape[1]
    share = heads // (q_ref.shape[2] // DK)
    every = range(heads)
    queries, keys, keys_t, met = [], [], [], []
    for at in range(0, q_ref.shape[2], DK):
        q = q_ref[0, :, at : at + DK].astype(F32)
        k = k_ref[0, :, at : at + DK].astype(F32)
        q = q * lax.rsqrt(jnp.sum(q * q, axis=-1, keepdims=True) + 1e-06) * DK ** (-0.5)
        k = k * lax.rsqrt(jnp.sum(k * k, axis=-1, keepdims=True) + 1e-06)
        queries.append(q)
        keys.append(k)
        keys_t.append(k.T)
        met.append(dot_split(jnp.concatenate([k, q], axis=0), keys_t[-1]))
    lower, scores, inverse = [], [], []
    for head in every:
        away = sum_col_ref[0, :, head : head + 1] - sum_row_ref[0, head : head + 1, :]
        ratio = jnp.where(row >= col, jnp.exp(jnp.where(row >= col, away, 0.0)), 0.0)
        pair = met[head // share]
        rate = rate_col_ref[0, :, head : head + 1]
        lower.append(jnp.where(row > col, rate * ratio * pair[:span], 0.0))
        scores.append(ratio * pair[span:])
    small = [jnp.where(row // 8 == col // 8, lower[h], 0.0) for h in every]
    square = [dot_split(small[h], small[h]) for h in every]
    inverse = [dot_split(ident - small[h], ident + square[h]) for h in every]
    fourth = [dot_split(square[h], square[h]) for h in every]
    inverse = [dot_split(inverse[h], ident + fourth[h]) for h in every]
    size = 8
    while size < span:
        between = (row // (2 * size) == col // (2 * size)) & (row // size != col // size)
        moved = [dot_split(jnp.where(between, lower[h], 0.0), inverse[h]) for h in every]
        inverse = [inverse[h] - dot_split(inverse[h], moved[h]) for h in every]
        size *= 2
    v_maps = []
    for head in every:
        sum_row = sum_row_ref[0, head : head + 1, :]
        tail = keys_t[head // share] * jnp.exp(sum_row[:, span - 1 : span] - sum_row)
        solve = inverse[head] * rate_row_ref[0, head : head + 1, :]
        v_maps.append(dot_split(jnp.concatenate([scores[head], tail], axis=0), solve))
        v_map_ref[0, head] = jnp.concatenate(halves(v_maps[-1]), axis=1)
    for head in every:
        growth = jnp.exp(sum_col_ref[0, :, head : head + 1])
        whole = jnp.exp(sum_row_ref[0, head : head + 1, span - 1 : span])
        fixed = jnp.concatenate([growth * queries[head // share], whole * ident], axis=0)
        s_map = fixed - dot_split(v_maps[head], growth * keys[head // share])
        s_map_ref[0, head] = jnp.concatenate(halves(s_map), axis=1)


def key_maps(*args):
    blocks, span, _ = args[0].shape
    heads = args[3].shape[1]
    out = jax.ShapeDtypeStruct((blocks, heads, span + DK, 2 * span), BF16)

    def whole(array):
        return pl.BlockSpec((1,) + array.shape[1:], lambda n: (n,) + (0,) * (array.ndim - 1))

    return pl.pallas_call(
        maps_body,
        grid=(blocks,),
        in_specs=[whole(a) for a in args],
        out_specs=[whole(out), whole(out)],
        out_shape=[out, out],
        name="key_maps",
    )(*args)


def order_body(at_ref, own_ref, other_ref, out_ref):
    n_x, n_z, rows, _ = own_ref.shape
    n_c = 2
    for z in range(n_z):
        for x in range(n_x):
            for c in range(n_c):
                place = ((z * n_x + x) * n_c + c) * rows
                at = (lax.rem(at_ref[1] - x + n_x, n_x), lax.rem(z - at_ref[0] + n_z, n_z))
                here, there = own_ref[at], other_ref[at]
                out_ref[place : place + rows, :] = jnp.where(at_ref[2] == c, here, there)


def finish_body(n_sa, me_ref, gain_ref, weight_ref, v_map_ref, s_map_ref, *refs):
    *streams, head_ref, normed_ref = refs
    _, tokens, own = head_ref.shape
    heads = v_map_ref.shape[1]
    width = normed_ref.shape[1]
    me = me_ref[0]
    gain = gain_ref[...].astype(F32)
    for s in range(n_sa):
        stream = jnp.concatenate([a[...] for a in streams[s::n_sa]], axis=1).astype(F32)
        scale = lax.rsqrt(jnp.sum(stream * stream, axis=-1, keepdims=True) / width + 1e-06)
        normed_ref[s * tokens : (s + 1) * tokens, :] = (stream * scale * gain).astype(BF16)

    @pl.loop(0, own, step=256)
    def _(at):
        lanes = pl.ds(pl.multiple_of(at, 256), 256)
        made = dot(normed_ref[...], weight_ref[:, lanes]).astype(BF16)
        for s in range(n_sa):
            head_ref[lax.rem(me - s + n_sa, n_sa), :, lanes] = made[s * tokens : (s + 1) * tokens]

    states = [None] * heads
    for n in range(n_sa):
        at = lax.rem(me - n + n_sa, n_sa)
        for head in range(heads):
            lanes = slice(head * DV, (head + 1) * DV)
            v = head_ref[n, :, lanes]
            out = dot(v_map_ref[at, head], jnp.concatenate([v, v], axis=0))
            if n > 0:
                high, low = halves(states[head])
                maps = s_map_ref[at, head]
                out = out + dot(maps, jnp.concatenate([high, high], axis=0))
                out = out + dot(maps[:, :DK], low)
            head_ref[n, :, lanes] = out[:tokens].astype(BF16)
            states[head] = out[tokens:]


def finish(me, gain, weight, v_map, s_map, streams, n_sa):
    tokens = streams[0].shape[0]
    width, own = weight.shape

    def body(*refs):
        finish_body(n_sa, *refs)

    return pl.pallas_call(
        body,
        in_specs=[SCALARS] + [WHOLE] * (4 + len(streams)),
        out_specs=WHOLE,
        out_shape=jax.ShapeDtypeStruct((n_sa, tokens, own), BF16),
        scratch_shapes=[pltpu.VMEM((n_sa * tokens, width), BF16)],
        name="finish",
    )(me, gain, weight, v_map, s_map, *streams)


def key_arguments(qk, extra, tokens):
    n_sa = qk.shape[0]
    heads = HV // n_sa
    rates = qk[:, tokens : tokens + extra].reshape(n_sa, 3, 2 * heads, tokens).astype(F32)
    rates = rates[:, 0] + rates[:, 1] + rates[:, 2]
    qk = qk[:, :tokens]
    until = (
        lax.broadcasted_iota(jnp.int32, (tokens, tokens), 0)
        <= lax.broadcasted_iota(jnp.int32, (tokens, tokens), 1)
    ).astype(F32)
    sum_row = jnp.einsum("nhp,pt->nht", rates[:, :heads], until, precision=HIGHEST)
    rate_row = rates[:, heads:]
    half = qk.shape[2] // 2
    return (
        qk[..., :half],
        qk[..., half:],
        sum_row.transpose(0, 2, 1),
        sum_row,
        rate_row.transpose(0, 2, 1),
        rate_row,
    )


def on_device(
    expert_hidden,
    down_weight,
    residual,
    expert_ids,
    combine_weight,
    norm_gain,
    value_weight,
    queries,
    keys,
    log_decay,
    write_rate,
):
    n_z, n_x, n_c, n_sa = (lax.axis_size(a) for a in ("z", "x", "c", "sa"))
    n_xc = n_x * n_c
    exp_dev, _, width = down_weight.shape
    tokens = residual.shape[1]
    top = expert_ids.shape[2]
    own = width // n_sa
    heads = HV // n_sa
    sa = lax.axis_index("sa")
    me = sa[None]

    hidden = ordered_hidden(expert_hidden, n_z, n_xc)
    made = produce(hidden, down_weight, 0, CHUNKS[0], n_xc)

    table = jnp.concatenate([expert_ids[0].astype(F32), combine_weight[0]], axis=1).T
    table = after(table.astype(BF16), made).reshape(-1, own)
    part = lax.dynamic_slice_in_dim(value_weight, sa * own, own, axis=1)
    rows, extra = part.shape[0], table.shape[0]
    packed = jnp.concatenate([part, table, jnp.zeros((-extra % 8, own), BF16)], axis=0)
    packed = gathered(packed, "z", -1)
    part = packed[:, :rows]
    tables = packed[:, rows : rows + extra].reshape(n_z, 2 * top, tokens).astype(F32)
    combine = combine_matrix(tables.transpose(0, 2, 1), top, exp_dev, n_xc)

    def by_group(array):
        return array[0].reshape(tokens, n_sa, -1).transpose(1, 0, 2)

    log_decay, write_rate, queries, keys = lax.optimization_barrier(
        (log_decay, write_rate, queries, keys, made)
    )[:4]
    rates = jnp.concatenate(
        [log_decay[0].T.reshape(n_sa, heads, tokens), write_rate[0].T.reshape(n_sa, heads, tokens)],
        axis=1,
    )
    rates = jnp.stack(thirds(rates), axis=1).reshape(n_sa, -1, own)
    extra = rates.shape[1]
    rates = jnp.pad(rates, ((0, 0), (0, -extra % 8), (0, 0)))
    sent = jnp.concatenate([by_group(queries), by_group(keys)], axis=2)
    sent = jnp.concatenate([sent, rates], axis=1)
    qk = []
    for s in range(n_sa):
        piece = lax.dynamic_index_in_dim(sent, (sa + s) % n_sa, keepdims=False)
        qk.append(shifted(piece, "sa", s) if s else piece)
    qk = jnp.stack(qk)

    starts = [sum(CHUNKS[:n]) for n in range(len(CHUNKS))]

    def add_up(number, parts):
        own_part = residual[0, :, starts[number] : starts[number] + CHUNKS[number]]
        return sum_rounded(own_part, *parts)

    def spread(stream):
        return [stream] + [shifted(stream, "sa", s) for s in range(1, n_sa)]

    def exchange(rows):
        return lax.all_to_all(rows, ("x", "c"), split_axis=0, concat_axis=0, tiled=True)

    def make(rows, number):
        return produce(rows, down_weight, starts[number], CHUNKS[number], n_xc)

    def gather_chunk(number, weighting, rows):
        return combine_rows(weighting, rows, n_z, number == 2)

    got = exchange(made)
    made = make(hidden, 1)
    made, qk, got = lax.optimization_barrier((made, qk, got))

    arrived = exchange(made)
    parts = gather_chunk(0, combine, got)
    first = start_sum_over_z(parts, True)
    made = make(after(hidden, parts[0]), 2)
    _, earlier = pass_on(*first, made)
    made, got = lax.optimization_barrier((made, arrived))

    arrived = exchange(made)
    parts = gather_chunk(1, combine, got)
    first = start_sum_over_z(parts, False)
    *earlier, _ = lax.optimization_barrier((*earlier, parts[0]))
    stream = add_up(0, earlier)
    sums, earlier = pass_on(*first, stream)
    combine, *_ = lax.optimization_barrier((combine, *sums))

    part = after(part, arrived)
    part = jnp.stack([part] + [shifted(part, "x", r) for r in range(1, n_x)])
    (parts,) = gather_chunk(2, combine, arrived)
    *earlier, _ = lax.optimization_barrier((*earlier, parts))
    streams = spread(jnp.concatenate([stream, add_up(1, earlier)], axis=1))
    v_map, s_map = key_maps(*key_arguments(after(qk, parts), extra, tokens))
    parts = lax.all_to_all(parts, "z", split_axis=0, concat_axis=0, tiled=True)
    parts, v_map, s_map = lax.optimization_barrier((parts, v_map, s_map))
    streams += spread(add_up(2, [parts[z] for z in range(n_z)]))
    place = jnp.stack([lax.axis_index(a) for a in ("z", "x", "c")])
    projection = pl.pallas_call(
        order_body,
        in_specs=[SCALARS, WHOLE, WHOLE],
        out_specs=WHOLE,
        out_shape=jax.ShapeDtypeStruct((width, own), BF16),
        name="order",
    )(place, part, shifted(part, "c", 1))
    out = finish(me, norm_gain[None], projection, v_map, s_map, streams, n_sa)
    out = lax.all_to_all(out, "sa", split_axis=0, concat_axis=0, tiled=True)
    return out.transpose(1, 0, 2).reshape(1, tokens, width)


def solution(mesh):
    fine = Mesh(mesh.devices.reshape(8, 4, 2, 4), ("z", "x", "c", "sa"))
    ea = ("z", "x", "c")
    return jax.shard_map(
        on_device,
        mesh=fine,
        in_specs=(
            P(ea, "sa", None),
            P(ea, None, None),
            P(ea, "sa", None),
            P(ea, "sa", None),
            P(ea, "sa", None),
            P(),
            P(ea, None),
            P(ea, "sa", None),
            P(ea, "sa", None),
            P(ea, "sa", None),
            P(ea, "sa", None),
        ),
        out_specs=P(ea, "sa", None),
        check_vma=False,
    )
```

```python
import jax
import jax.numpy as jnp
from jax import lax
from jax.experimental import pallas as pl
from jax.experimental.pallas import tpu as pltpu
from jax.sharding import Mesh, PartitionSpec as P


HV = 16
DK = 128
DV = 128
CAP = 7
CHUNKS = (768, 768, 512)
HIGHEST = lax.Precision.HIGHEST
F32 = jnp.float32
BF16 = jnp.bfloat16
WHOLE = pl.BlockSpec(memory_space=pltpu.VMEM)
SCALARS = pl.BlockSpec(memory_space=pltpu.SMEM)


def dot(a, b):
    return jnp.dot(a, b, preferred_element_type=F32)


def halves(x):
    high = x.astype(BF16)
    return high, (x - high.astype(F32)).astype(BF16)


def dot_split(a, b):
    a_high, a_low = halves(a)
    b_high, b_low = halves(b)
    both = jnp.concatenate([a_high, a_low], axis=1)
    return dot(both, jnp.concatenate([b_high, b_high], axis=0)) + dot(a_high, b_low)


def shifted(array, axis, by):
    names = axis if isinstance(axis, tuple) else (axis,)
    count = 1
    for name in names:
        count *= lax.axis_size(name)
    return lax.ppermute(array, axis, [(i, (i + by) % count) for i in range(count)])


def after(value, *others):
    return lax.optimization_barrier((value,) + others)[0]


def gathered(array, axis, sign=1):
    held, by = array[None], 1
    while by < lax.axis_size(axis):
        moved = shifted(held, axis, sign * by)
        held = jnp.concatenate([held, moved], axis=0)
        by *= 2
    return held


def thirds(x):
    pieces = []
    for _ in range(3):
        piece = lax.reduce_precision(x, 8, 7)
        pieces.append(piece.astype(BF16))
        x = x - piece
    return pieces


def ordered_hidden(expert_hidden, n_z, n_xc):
    experts, rows, _ = expert_hidden.shape
    half = n_z // 2
    used = half * CAP
    padded = n_xc * 2 * 32
    at = lax.broadcasted_iota(jnp.int32, (experts, padded, 1), 1)
    odd = lax.broadcasted_iota(jnp.int32, (experts, padded, 1), 0) % 2
    inner = at % 32 - odd * (32 - used)
    z = (lax.axis_index("z") + at // 32 % 2 * half + inner // CAP) % n_z
    xc = at // 64
    source = jnp.where((inner >= 0) & (inner < used), (z * n_xc + xc) * CAP + inner % CAP, -1)
    order = (source == lax.broadcasted_iota(jnp.int32, (1, 1, rows), 2)).astype(BF16)
    return jnp.einsum(
        "epr,erf->epf", order, expert_hidden, preferred_element_type=F32
    ).astype(BF16)


def produce_body(hidden_ref, weight_ref, out_ref):
    experts = hidden_ref.shape[0]
    made = [dot(hidden_ref[e], weight_ref[e]) for e in range(experts)]
    for group in range(out_ref.shape[0]):
        for half in range(2):
            at = (group * 2 + half) * 32
            pieces = []
            for e in range(0, experts, 2):
                a, b = made[e][at : at + 32], made[e + 1][at : at + 32]
                pieces += [a[:24], a[24:] + b[:8], b[8:]]
            rows = jnp.concatenate(pieces, axis=0)
            span = rows.shape[0]
            out_ref[group, half * span : (half + 1) * span, :] = rows.astype(BF16)


def produce(hidden, weight, start, cols, n_xc):
    experts, rows, units = hidden.shape
    block = 128
    while start % (2 * block) == 0 and cols % (2 * block) == 0 and block < 256:
        block *= 2
    sent = experts * 28 * 2
    return pl.pallas_call(
        produce_body,
        grid=(cols // block,),
        in_specs=[
            pl.BlockSpec((experts, rows, units), lambda n: (0, 0, 0)),
            pl.BlockSpec((experts, units, block), lambda n: (0, 0, start // block + n)),
        ],
        out_specs=pl.BlockSpec((n_xc, sent, block), lambda n: (0, 0, n)),
        out_shape=jax.ShapeDtypeStruct((n_xc, sent, cols), BF16),
        name="produce",
    )(hidden, weight)


def combine_matrix(tables, top, experts_of, n_xc):
    n_z, tokens, _ = tables.shape
    half = n_z // 2
    experts = experts_of * n_xc
    ids, weights = tables[..., :top], tables[..., top:]
    base = (lax.axis_index("z") * experts).astype(F32)
    named = ids[..., None] == base + jnp.arange(experts, dtype=F32)
    counts = jnp.sum(named.astype(F32), axis=2)
    dense = jnp.sum(jnp.where(named, weights[..., None], 0.0), axis=2).astype(BF16)
    earlier = (
        lax.broadcasted_iota(jnp.int32, (tokens, tokens), 0)
        > lax.broadcasted_iota(jnp.int32, (tokens, tokens), 1)
    ).astype(BF16)
    prior = jnp.einsum("tp,zpe->zte", earlier, counts.astype(BF16), preferred_element_type=F32)
    each = experts_of * half * CAP
    rows = each * n_xc
    at = lax.broadcasted_iota(jnp.int32, (experts, rows), 1)
    owner = at // (half * CAP)
    pick = (owner == lax.broadcasted_iota(jnp.int32, (experts, rows), 0)).astype(BF16)
    prior_rows = jnp.einsum("zte,er->ztr", prior.astype(BF16), pick, preferred_element_type=F32)
    dense_rows = jnp.einsum("zte,er->ztr", dense, pick, preferred_element_type=F32)
    at = lax.broadcasted_iota(jnp.int32, (n_z, 1, rows), 2)
    mine = at % (half * CAP) // CAP == lax.broadcasted_iota(jnp.int32, (n_z, 1, rows), 0) % half
    hit = mine & (prior_rows == (at % CAP).astype(F32))
    return jnp.where(hit, dense_rows, 0.0).astype(BF16).reshape(2, half * tokens, rows)


def combine_body(me_ref, combine_ref, got_ref, *outs):
    n_xc, rows, cols = got_ref.shape
    rows //= 2
    tokens = outs[0].shape[-2]
    half = combine_ref.shape[1] // tokens
    for h in range(2):
        filled = got_ref[:, h * rows : (h + 1) * rows, :].reshape(n_xc * rows, cols)
        sums = dot(combine_ref[h], filled)
        for z in range(half):
            rounded = sums[z * tokens : (z + 1) * tokens].astype(BF16)
            if len(outs) == 1:
                outs[0][lax.rem(me_ref[0] + h * half + z, 2 * half)] = rounded
            else:
                outs[h * half + z][...] = rounded


def combine_rows(combine, got, n_z, stacked):
    tokens = combine.shape[1] * 2 // n_z
    cols = got.shape[2]
    block = 256
    if stacked:
        outs = [jax.ShapeDtypeStruct((n_z, tokens, cols), BF16)]
        specs = [pl.BlockSpec((n_z, tokens, block), lambda n: (0, 0, n))]
    else:
        outs = [jax.ShapeDtypeStruct((tokens, cols), BF16)] * n_z
        specs = [pl.BlockSpec((tokens, block), lambda n: (0, n))] * n_z
    return pl.pallas_call(
        combine_body,
        grid=(cols // block,),
        in_specs=[
            SCALARS,
            pl.BlockSpec(combine.shape, lambda n: (0, 0, 0)),
            pl.BlockSpec(got.shape[:2] + (block,), lambda n: (0, 0, n)),
        ],
        out_specs=specs,
        out_shape=outs,
        name="combine",
    )(lax.axis_index("z")[None], combine, got)


def sum_rounded(*parts):
    total = parts[0].astype(F32)
    for part in parts[1:]:
        total = total + part.astype(F32)
    return total.astype(BF16)


def start_sum_over_z(parts, upward):
    up = shifted(parts[3], "z", 1)
    down = shifted(parts[5], "z", -1)
    far = shifted(parts[4], "z", 2 if upward else -2)
    plus = [parts[2], up] + ([far] if upward else [])
    minus = [parts[6], down] + ([] if upward else [far])
    near = [shifted(parts[1], "z", 1), shifted(parts[7], "z", -1)]
    return plus, minus, [parts[0]] + near


def pass_on(plus, minus, near, gate):
    *plus, _ = lax.optimization_barrier((*plus, gate))
    *minus, _ = lax.optimization_barrier((*minus, gate))
    sums = [sum_rounded(*plus), sum_rounded(*minus)]
    return sums, near + [shifted(sums[0], "z", 2), shifted(sums[1], "z", -2)]


def maps_body(q_ref, k_ref, sum_col_ref, sum_row_ref, rate_col_ref, rate_row_ref, v_map_ref, s_map_ref):
    span = q_ref.shape[1]
    row = lax.broadcasted_iota(jnp.int32, (span, span), 0)
    col = lax.broadcasted_iota(jnp.int32, (span, span), 1)
    ident = (row == col).astype(F32)
    heads = v_map_ref.shape[1]
    share = heads // (q_ref.shape[2] // DK)
    every = range(heads)
    queries, keys, keys_t, met = [], [], [], []
    for at in range(0, q_ref.shape[2], DK):
        q = q_ref[0, :, at : at + DK].astype(F32)
        k = k_ref[0, :, at : at + DK].astype(F32)
        q = q * lax.rsqrt(jnp.sum(q * q, axis=-1, keepdims=True) + 1e-06) * DK ** (-0.5)
        k = k * lax.rsqrt(jnp.sum(k * k, axis=-1, keepdims=True) + 1e-06)
        queries.append(q)
        keys.append(k)
        keys_t.append(k.T)
        met.append(dot_split(jnp.concatenate([k, q], axis=0), keys_t[-1]))
    lower, scores, inverse = [], [], []
    for head in every:
        away = sum_col_ref[0, :, head : head + 1] - sum_row_ref[0, head : head + 1, :]
        ratio = jnp.where(row >= col, jnp.exp(jnp.where(row >= col, away, 0.0)), 0.0)
        pair = met[head // share]
        rate = rate_col_ref[0, :, head : head + 1]
        lower.append(jnp.where(row > col, rate * ratio * pair[:span], 0.0))
        scores.append(ratio * pair[span:])
    small = [jnp.where(row // 8 == col // 8, lower[h], 0.0) for h in every]
    square = [dot_split(small[h], small[h]) for h in every]
    inverse = [dot_split(ident - small[h], ident + square[h]) for h in every]
    fourth = [dot_split(square[h], square[h]) for h in every]
    inverse = [dot_split(inverse[h], ident + fourth[h]) for h in every]
    size = 8
    while size < span:
        between = (row // (2 * size) == col // (2 * size)) & (row // size != col // size)
        moved = [dot_split(jnp.where(between, lower[h], 0.0), inverse[h]) for h in every]
        inverse = [inverse[h] - dot_split(inverse[h], moved[h]) for h in every]
        size *= 2
    v_maps = []
    for head in every:
        sum_row = sum_row_ref[0, head : head + 1, :]
        tail = keys_t[head // share] * jnp.exp(sum_row[:, span - 1 : span] - sum_row)
        solve = inverse[head] * rate_row_ref[0, head : head + 1, :]
        v_maps.append(dot_split(jnp.concatenate([scores[head], tail], axis=0), solve))
        v_map_ref[0, head] = jnp.concatenate(halves(v_maps[-1]), axis=1)
    for head in every:
        growth = jnp.exp(sum_col_ref[0, :, head : head + 1])
        whole = jnp.exp(sum_row_ref[0, head : head + 1, span - 1 : span])
        fixed = jnp.concatenate([growth * queries[head // share], whole * ident], axis=0)
        s_map = fixed - dot_split(v_maps[head], growth * keys[head // share])
        s_map_ref[0, head] = jnp.concatenate(halves(s_map), axis=1)


def key_maps(*args):
    blocks, span, _ = args[0].shape
    heads = args[3].shape[1]
    out = jax.ShapeDtypeStruct((blocks, heads, span + DK, 2 * span), BF16)

    def whole(array):
        return pl.BlockSpec((1,) + array.shape[1:], lambda n: (n,) + (0,) * (array.ndim - 1))

    return pl.pallas_call(
        maps_body,
        grid=(blocks,),
        in_specs=[whole(a) for a in args],
        out_specs=[whole(out), whole(out)],
        out_shape=[out, out],
        name="key_maps",
    )(*args)


def order_body(at_ref, own_ref, other_ref, out_ref):
    n_x, n_z, rows, _ = own_ref.shape
    n_c = 2
    for z in range(n_z):
        for x in range(n_x):
            for c in range(n_c):
                place = ((z * n_x + x) * n_c + c) * rows
                at = (lax.rem(at_ref[1] - x + n_x, n_x), lax.rem(z - at_ref[0] + n_z, n_z))
                here, there = own_ref[at], other_ref[at]
                out_ref[place : place + rows, :] = jnp.where(at_ref[2] == c, here, there)


def finish_body(n_sa, me_ref, gain_ref, weight_ref, v_map_ref, s_map_ref, *refs):
    *streams, head_ref, normed_ref = refs
    _, tokens, own = head_ref.shape
    heads = v_map_ref.shape[1]
    width = normed_ref.shape[1]
    me = me_ref[0]
    gain = gain_ref[...].astype(F32)
    for s in range(n_sa):
        stream = jnp.concatenate([a[...] for a in streams[s::n_sa]], axis=1).astype(F32)
        scale = lax.rsqrt(jnp.sum(stream * stream, axis=-1, keepdims=True) / width + 1e-06)
        normed_ref[s * tokens : (s + 1) * tokens, :] = (stream * scale * gain).astype(BF16)

    @pl.loop(0, own, step=256)
    def _(at):
        lanes = pl.ds(pl.multiple_of(at, 256), 256)
        made = dot(normed_ref[...], weight_ref[:, lanes]).astype(BF16)
        for s in range(n_sa):
            head_ref[lax.rem(me - s + n_sa, n_sa), :, lanes] = made[s * tokens : (s + 1) * tokens]

    states = [None] * heads
    for n in range(n_sa):
        at = lax.rem(me - n + n_sa, n_sa)
        for head in range(heads):
            lanes = slice(head * DV, (head + 1) * DV)
            v = head_ref[n, :, lanes]
            out = dot(v_map_ref[at, head], jnp.concatenate([v, v], axis=0))
            if n > 0:
                high, low = halves(states[head])
                maps = s_map_ref[at, head]
                out = out + dot(maps, jnp.concatenate([high, high], axis=0))
                out = out + dot(maps[:, :DK], low)
            head_ref[n, :, lanes] = out[:tokens].astype(BF16)
            states[head] = out[tokens:]


def finish(me, gain, weight, v_map, s_map, streams, n_sa):
    tokens = streams[0].shape[0]
    width, own = weight.shape

    def body(*refs):
        finish_body(n_sa, *refs)

    return pl.pallas_call(
        body,
        in_specs=[SCALARS] + [WHOLE] * (4 + len(streams)),
        out_specs=WHOLE,
        out_shape=jax.ShapeDtypeStruct((n_sa, tokens, own), BF16),
        scratch_shapes=[pltpu.VMEM((n_sa * tokens, width), BF16)],
        name="finish",
    )(me, gain, weight, v_map, s_map, *streams)


def key_arguments(qk, extra, tokens):
    n_sa = qk.shape[0]
    heads = HV // n_sa
    rates = qk[:, tokens : tokens + extra].reshape(n_sa, 3, 2 * heads, tokens).astype(F32)
    rates = rates[:, 0] + rates[:, 1] + rates[:, 2]
    qk = qk[:, :tokens]
    until = (
        lax.broadcasted_iota(jnp.int32, (tokens, tokens), 0)
        <= lax.broadcasted_iota(jnp.int32, (tokens, tokens), 1)
    ).astype(F32)
    sum_row = jnp.einsum("nhp,pt->nht", rates[:, :heads], until, precision=HIGHEST)
    rate_row = rates[:, heads:]
    half = qk.shape[2] // 2
    return (
        qk[..., :half],
        qk[..., half:],
        sum_row.transpose(0, 2, 1),
        sum_row,
        rate_row.transpose(0, 2, 1),
        rate_row,
    )


def on_device(
    expert_hidden,
    down_weight,
    residual,
    expert_ids,
    combine_weight,
    norm_gain,
    value_weight,
    queries,
    keys,
    log_decay,
    write_rate,
):
    n_z, n_x, n_c, n_sa = (lax.axis_size(a) for a in ("z", "x", "c", "sa"))
    n_xc = n_x * n_c
    exp_dev, _, width = down_weight.shape
    tokens = residual.shape[1]
    top = expert_ids.shape[2]
    own = width // n_sa
    heads = HV // n_sa
    sa = lax.axis_index("sa")
    me = sa[None]

    hidden = ordered_hidden(expert_hidden, n_z, n_xc)
    made = produce(hidden, down_weight, 0, CHUNKS[0], n_xc)

    table = jnp.concatenate([expert_ids[0].astype(F32), combine_weight[0]], axis=1).T
    table = after(table.astype(BF16), made).reshape(-1, own)
    part = lax.dynamic_slice_in_dim(value_weight, sa * own, own, axis=1)
    rows, extra = part.shape[0], table.shape[0]
    packed = jnp.concatenate([part, table, jnp.zeros((-extra % 8, own), BF16)], axis=0)
    packed = gathered(packed, "z", -1)
    part = packed[:, :rows]
    tables = packed[:, rows : rows + extra].reshape(n_z, 2 * top, tokens).astype(F32)
    combine = combine_matrix(tables.transpose(0, 2, 1), top, exp_dev, n_xc)

    def by_group(array):
        return array[0].reshape(tokens, n_sa, -1).transpose(1, 0, 2)

    log_decay, write_rate, queries, keys = lax.optimization_barrier(
        (log_decay, write_rate, queries, keys, made)
    )[:4]
    rates = jnp.concatenate(
        [log_decay[0].T.reshape(n_sa, heads, tokens), write_rate[0].T.reshape(n_sa, heads, tokens)],
        axis=1,
    )
    rates = jnp.stack(thirds(rates), axis=1).reshape(n_sa, -1, own)
    extra = rates.shape[1]
    rates = jnp.pad(rates, ((0, 0), (0, -extra % 8), (0, 0)))
    sent = jnp.concatenate([by_group(queries), by_group(keys)], axis=2)
    sent = jnp.concatenate([sent, rates], axis=1)
    qk = []
    for s in range(n_sa):
        piece = lax.dynamic_index_in_dim(sent, (sa + s) % n_sa, keepdims=False)
        qk.append(shifted(piece, "sa", s) if s else piece)
    qk = jnp.stack(qk)

    starts = [sum(CHUNKS[:n]) for n in range(len(CHUNKS))]

    def add_up(number, parts):
        own_part = residual[0, :, starts[number] : starts[number] + CHUNKS[number]]
        return sum_rounded(own_part, *parts)

    def spread(stream):
        return [stream] + [shifted(stream, "sa", s) for s in range(1, n_sa)]

    def exchange(rows):
        return lax.all_to_all(rows, ("x", "c"), split_axis=0, concat_axis=0, tiled=True)

    def make(rows, number):
        return produce(rows, down_weight, starts[number], CHUNKS[number], n_xc)

    def gather_chunk(number, weighting, rows):
        return combine_rows(weighting, rows, n_z, number == 2)

    got = exchange(made)
    made = make(hidden, 1)
    v_map, s_map = key_maps(*key_arguments(qk, extra, tokens))
    made, v_map, s_map, got = lax.optimization_barrier((made, v_map, s_map, got))

    arrived = exchange(made)
    parts = gather_chunk(0, combine, got)
    first = start_sum_over_z(parts, True)
    made = make(after(hidden, parts[0]), 2)
    _, earlier = pass_on(*first, made)
    made, got = lax.optimization_barrier((made, arrived))

    arrived = exchange(made)
    parts = gather_chunk(1, combine, got)
    first = start_sum_over_z(parts, False)
    *earlier, _ = lax.optimization_barrier((*earlier, parts[0]))
    stream = add_up(0, earlier)
    sums, earlier = pass_on(*first, stream)
    combine, *_ = lax.optimization_barrier((combine, *sums))

    part = after(part, arrived)
    part = jnp.stack([part] + [shifted(part, "x", r) for r in range(1, n_x)])
    (parts,) = gather_chunk(2, combine, arrived)
    *earlier, _ = lax.optimization_barrier((*earlier, parts))
    streams = spread(jnp.concatenate([stream, add_up(1, earlier)], axis=1))
    parts = lax.all_to_all(parts, "z", split_axis=0, concat_axis=0, tiled=True)
    streams += spread(add_up(2, [parts[z] for z in range(n_z)]))
    other = shifted(part, "c", 1)
    place = jnp.stack([lax.axis_index(a) for a in ("z", "x", "c")])
    projection = pl.pallas_call(
        order_body,
        in_specs=[SCALARS, WHOLE, WHOLE],
        out_specs=WHOLE,
        out_shape=jax.ShapeDtypeStruct((width, own), BF16),
        name="order",
    )(place, part, other)
    out = finish(me, norm_gain[None], projection, v_map, s_map, streams, n_sa)
    out = lax.all_to_all(out, "sa", split_axis=0, concat_axis=0, tiled=True)
    return out.transpose(1, 0, 2).reshape(1, tokens, width)


def solution(mesh):
    fine = Mesh(mesh.devices.reshape(8, 4, 2, 4), ("z", "x", "c", "sa"))
    ea = ("z", "x", "c")
    return jax.shard_map(
        on_device,
        mesh=fine,
        in_specs=(
            P(ea, "sa", None),
            P(ea, None, None),
            P(ea, "sa", None),
            P(ea, "sa", None),
            P(ea, "sa", None),
            P(),
            P(ea, None),
            P(ea, "sa", None),
            P(ea, "sa", None),
            P(ea, "sa", None),
            P(ea, "sa", None),
        ),
        out_specs=P(ea, "sa", None),
        check_vma=False,
    )
```

```python
import jax
import jax.numpy as jnp
from jax import lax
from jax.experimental import pallas as pl
from jax.experimental.pallas import tpu as pltpu
from jax.sharding import Mesh, PartitionSpec as P


HV = 16
DK = 128
DV = 128
CAP = 7
CHUNKS = (768, 768, 512)
HIGHEST = lax.Precision.HIGHEST
F32 = jnp.float32
BF16 = jnp.bfloat16
WHOLE = pl.BlockSpec(memory_space=pltpu.VMEM)
SCALARS = pl.BlockSpec(memory_space=pltpu.SMEM)


def dot(a, b):
    return jnp.dot(a, b, preferred_element_type=F32)


def halves(x):
    high = x.astype(BF16)
    return high, (x - high.astype(F32)).astype(BF16)


def dot_split(a, b):
    a_high, a_low = halves(a)
    b_high, b_low = halves(b)
    both = jnp.concatenate([a_high, a_low], axis=1)
    return dot(both, jnp.concatenate([b_high, b_high], axis=0)) + dot(a_high, b_low)


def shifted(array, axis, by):
    names = axis if isinstance(axis, tuple) else (axis,)
    count = 1
    for name in names:
        count *= lax.axis_size(name)
    return lax.ppermute(array, axis, [(i, (i + by) % count) for i in range(count)])


def after(value, *others):
    return lax.optimization_barrier((value,) + others)[0]


def gathered(array, axis, sign=1):
    held, by = array[None], 1
    while by < lax.axis_size(axis):
        moved = shifted(held, axis, sign * by)
        held = jnp.concatenate([held, moved], axis=0)
        by *= 2
    return held


def thirds(x):
    pieces = []
    for _ in range(3):
        piece = lax.reduce_precision(x, 8, 7)
        pieces.append(piece.astype(BF16))
        x = x - piece
    return pieces


def ordered_hidden(expert_hidden, n_z, n_xc):
    experts, rows, _ = expert_hidden.shape
    half = n_z // 2
    used = half * CAP
    padded = n_xc * 2 * 32
    at = lax.broadcasted_iota(jnp.int32, (experts, padded, 1), 1)
    odd = lax.broadcasted_iota(jnp.int32, (experts, padded, 1), 0) % 2
    inner = at % 32 - odd * (32 - used)
    z = (lax.axis_index("z") + at // 32 % 2 * half + inner // CAP) % n_z
    xc = at // 64
    source = jnp.where((inner >= 0) & (inner < used), (z * n_xc + xc) * CAP + inner % CAP, -1)
    order = (source == lax.broadcasted_iota(jnp.int32, (1, 1, rows), 2)).astype(BF16)
    return jnp.einsum(
        "epr,erf->epf", order, expert_hidden, preferred_element_type=F32
    ).astype(BF16)


def produce_body(hidden_ref, weight_ref, out_ref):
    experts = hidden_ref.shape[0]
    made = [dot(hidden_ref[e], weight_ref[e]) for e in range(experts)]
    for group in range(out_ref.shape[0]):
        for half in range(2):
            at = (group * 2 + half) * 32
            pieces = []
            for e in range(0, experts, 2):
                a, b = made[e][at : at + 32], made[e + 1][at : at + 32]
                pieces += [a[:24], a[24:] + b[:8], b[8:]]
            rows = jnp.concatenate(pieces, axis=0)
            span = rows.shape[0]
            out_ref[group, half * span : (half + 1) * span, :] = rows.astype(BF16)


def produce(hidden, weight, start, cols, n_xc):
    experts, rows, units = hidden.shape
    block = 128
    while start % (2 * block) == 0 and cols % (2 * block) == 0 and block < 256:
        block *= 2
    sent = experts * 28 * 2
    return pl.pallas_call(
        produce_body,
        grid=(cols // block,),
        in_specs=[
            pl.BlockSpec((experts, rows, units), lambda n: (0, 0, 0)),
            pl.BlockSpec((experts, units, block), lambda n: (0, 0, start // block + n)),
        ],
        out_specs=pl.BlockSpec((n_xc, sent, block), lambda n: (0, 0, n)),
        out_shape=jax.ShapeDtypeStruct((n_xc, sent, cols), BF16),
        name="produce",
    )(hidden, weight)


def combine_matrix(tables, top, experts_of, n_xc):
    n_z, tokens, _ = tables.shape
    half = n_z // 2
    experts = experts_of * n_xc
    ids, weights = tables[..., :top], tables[..., top:]
    base = (lax.axis_index("z") * experts).astype(F32)
    named = ids[..., None] == base + jnp.arange(experts, dtype=F32)
    counts = jnp.sum(named.astype(F32), axis=2)
    dense = jnp.sum(jnp.where(named, weights[..., None], 0.0), axis=2).astype(BF16)
    earlier = (
        lax.broadcasted_iota(jnp.int32, (tokens, tokens), 0)
        > lax.broadcasted_iota(jnp.int32, (tokens, tokens), 1)
    ).astype(BF16)
    prior = jnp.einsum("tp,zpe->zte", earlier, counts.astype(BF16), preferred_element_type=F32)
    each = experts_of * half * CAP
    rows = each * n_xc
    at = lax.broadcasted_iota(jnp.int32, (experts, rows), 1)
    owner = at // (half * CAP)
    pick = (owner == lax.broadcasted_iota(jnp.int32, (experts, rows), 0)).astype(BF16)
    prior_rows = jnp.einsum("zte,er->ztr", prior.astype(BF16), pick, preferred_element_type=F32)
    dense_rows = jnp.einsum("zte,er->ztr", dense, pick, preferred_element_type=F32)
    at = lax.broadcasted_iota(jnp.int32, (n_z, 1, rows), 2)
    mine = at % (half * CAP) // CAP == lax.broadcasted_iota(jnp.int32, (n_z, 1, rows), 0) % half
    hit = mine & (prior_rows == (at % CAP).astype(F32))
    return jnp.where(hit, dense_rows, 0.0).astype(BF16).reshape(2, half * tokens, rows)


def combine_body(me_ref, combine_ref, got_ref, *outs):
    n_xc, rows, cols = got_ref.shape
    rows //= 2
    tokens = outs[0].shape[-2]
    half = combine_ref.shape[1] // tokens
    for h in range(2):
        filled = got_ref[:, h * rows : (h + 1) * rows, :].reshape(n_xc * rows, cols)
        sums = dot(combine_ref[h], filled)
        for z in range(half):
            rounded = sums[z * tokens : (z + 1) * tokens].astype(BF16)
            if len(outs) == 1:
                outs[0][lax.rem(me_ref[0] + h * half + z, 2 * half)] = rounded
            else:
                outs[h * half + z][...] = rounded


def combine_rows(combine, got, n_z, stacked):
    tokens = combine.shape[1] * 2 // n_z
    cols = got.shape[2]
    block = 256
    if stacked:
        outs = [jax.ShapeDtypeStruct((n_z, tokens, cols), BF16)]
        specs = [pl.BlockSpec((n_z, tokens, block), lambda n: (0, 0, n))]
    else:
        outs = [jax.ShapeDtypeStruct((tokens, cols), BF16)] * n_z
        specs = [pl.BlockSpec((tokens, block), lambda n: (0, n))] * n_z
    return pl.pallas_call(
        combine_body,
        grid=(cols // block,),
        in_specs=[
            SCALARS,
            pl.BlockSpec(combine.shape, lambda n: (0, 0, 0)),
            pl.BlockSpec(got.shape[:2] + (block,), lambda n: (0, 0, n)),
        ],
        out_specs=specs,
        out_shape=outs,
        name="combine",
    )(lax.axis_index("z")[None], combine, got)


def sum_rounded(*parts):
    total = parts[0].astype(F32)
    for part in parts[1:]:
        total = total + part.astype(F32)
    return total.astype(BF16)


def start_sum_over_z(parts, upward):
    up = shifted(parts[3], "z", 1)
    down = shifted(parts[5], "z", -1)
    far = shifted(parts[4], "z", 2 if upward else -2)
    plus = [parts[2], up] + ([far] if upward else [])
    minus = [parts[6], down] + ([] if upward else [far])
    near = [shifted(parts[1], "z", 1), shifted(parts[7], "z", -1)]
    return plus, minus, [parts[0]] + near


def pass_on(plus, minus, near, gate):
    *plus, _ = lax.optimization_barrier((*plus, gate))
    *minus, _ = lax.optimization_barrier((*minus, gate))
    sums = [sum_rounded(*plus), sum_rounded(*minus)]
    return sums, near + [shifted(sums[0], "z", 2), shifted(sums[1], "z", -2)]


def maps_body(q_ref, k_ref, sum_col_ref, sum_row_ref, rate_col_ref, rate_row_ref, v_map_ref, s_map_ref):
    span = q_ref.shape[1]
    row = lax.broadcasted_iota(jnp.int32, (span, span), 0)
    col = lax.broadcasted_iota(jnp.int32, (span, span), 1)
    ident = (row == col).astype(F32)
    heads = v_map_ref.shape[1]
    share = heads // (q_ref.shape[2] // DK)
    every = range(heads)
    queries, keys, keys_t, met = [], [], [], []
    for at in range(0, q_ref.shape[2], DK):
        q = q_ref[0, :, at : at + DK].astype(F32)
        k = k_ref[0, :, at : at + DK].astype(F32)
        q = q * lax.rsqrt(jnp.sum(q * q, axis=-1, keepdims=True) + 1e-06) * DK ** (-0.5)
        k = k * lax.rsqrt(jnp.sum(k * k, axis=-1, keepdims=True) + 1e-06)
        queries.append(q)
        keys.append(k)
        keys_t.append(k.T)
        met.append(dot_split(jnp.concatenate([k, q], axis=0), keys_t[-1]))
    lower, scores, inverse = [], [], []
    for head in every:
        away = sum_col_ref[0, :, head : head + 1] - sum_row_ref[0, head : head + 1, :]
        ratio = jnp.where(row >= col, jnp.exp(jnp.where(row >= col, away, 0.0)), 0.0)
        pair = met[head // share]
        rate = rate_col_ref[0, :, head : head + 1]
        lower.append(jnp.where(row > col, rate * ratio * pair[:span], 0.0))
        scores.append(ratio * pair[span:])
    small = [jnp.where(row // 8 == col // 8, lower[h], 0.0) for h in every]
    square = [dot_split(small[h], small[h]) for h in every]
    inverse = [dot_split(ident - small[h], ident + square[h]) for h in every]
    fourth = [dot_split(square[h], square[h]) for h in every]
    inverse = [dot_split(inverse[h], ident + fourth[h]) for h in every]
    size = 8
    while size < span:
        between = (row // (2 * size) == col // (2 * size)) & (row // size != col // size)
        moved = [dot_split(jnp.where(between, lower[h], 0.0), inverse[h]) for h in every]
        inverse = [inverse[h] - dot_split(inverse[h], moved[h]) for h in every]
        size *= 2
    v_maps = []
    for head in every:
        sum_row = sum_row_ref[0, head : head + 1, :]
        tail = keys_t[head // share] * jnp.exp(sum_row[:, span - 1 : span] - sum_row)
        solve = inverse[head] * rate_row_ref[0, head : head + 1, :]
        v_maps.append(dot_split(jnp.concatenate([scores[head], tail], axis=0), solve))
        v_map_ref[0, head] = jnp.concatenate(halves(v_maps[-1]), axis=1)
    for head in every:
        growth = jnp.exp(sum_col_ref[0, :, head : head + 1])
        whole = jnp.exp(sum_row_ref[0, head : head + 1, span - 1 : span])
        fixed = jnp.concatenate([growth * queries[head // share], whole * ident], axis=0)
        s_map = fixed - dot_split(v_maps[head], growth * keys[head // share])
        s_map_ref[0, head] = jnp.concatenate(halves(s_map), axis=1)


def key_maps(*args):
    blocks, span, _ = args[0].shape
    heads = args[3].shape[1]
    out = jax.ShapeDtypeStruct((blocks, heads, span + DK, 2 * span), BF16)

    def whole(array):
        return pl.BlockSpec((1,) + array.shape[1:], lambda n: (n,) + (0,) * (array.ndim - 1))

    return pl.pallas_call(
        maps_body,
        grid=(blocks,),
        in_specs=[whole(a) for a in args],
        out_specs=[whole(out), whole(out)],
        out_shape=[out, out],
        name="key_maps",
    )(*args)


def order_body(at_ref, own_ref, other_ref, out_ref):
    n_x, n_z, rows, _ = own_ref.shape
    n_c = 2
    for z in range(n_z):
        for x in range(n_x):
            for c in range(n_c):
                place = ((z * n_x + x) * n_c + c) * rows
                at = (lax.rem(at_ref[1] - x + n_x, n_x), lax.rem(z - at_ref[0] + n_z, n_z))
                here, there = own_ref[at], other_ref[at]
                out_ref[place : place + rows, :] = jnp.where(at_ref[2] == c, here, there)


def finish_body(n_sa, me_ref, gain_ref, weight_ref, v_map_ref, s_map_ref, *refs):
    streams, outs = refs[: -n_sa - 2], refs[-n_sa - 2 : -2]
    normed_ref, head_ref = refs[-2:]
    tokens, own = outs[0].shape
    heads = v_map_ref.shape[1]
    width = normed_ref.shape[1]
    me = me_ref[0]
    gain = gain_ref[...].astype(F32)
    for s in range(n_sa):
        stream = jnp.concatenate([a[...] for a in streams[s::n_sa]], axis=1).astype(F32)
        scale = lax.rsqrt(jnp.sum(stream * stream, axis=-1, keepdims=True) / width + 1e-06)
        normed_ref[s * tokens : (s + 1) * tokens, :] = (stream * scale * gain).astype(BF16)

    @pl.loop(0, own, step=256)
    def _(at):
        lanes = pl.ds(pl.multiple_of(at, 256), 256)
        made = dot(normed_ref[...], weight_ref[:, lanes]).astype(BF16)
        for s in range(n_sa):
            head_ref[lax.rem(me - s + n_sa, n_sa), :, lanes] = made[s * tokens : (s + 1) * tokens]

    states = [None] * heads
    for n in range(n_sa):
        at = lax.rem(me - n + n_sa, n_sa)
        for head in range(heads):
            lanes = slice(head * DV, (head + 1) * DV)
            v = head_ref[n, :, lanes]
            out = dot(v_map_ref[at, head], jnp.concatenate([v, v], axis=0))
            if n > 0:
                high, low = halves(states[head])
                maps = s_map_ref[at, head]
                out = out + dot(maps, jnp.concatenate([high, high], axis=0))
                out = out + dot(maps[:, :DK], low)
            head_ref[n, :, lanes] = out[:tokens].astype(BF16)
            states[head] = out[tokens:]
    for s in range(n_sa):
        outs[s][...] = head_ref[lax.rem(me + s, n_sa)]


def finish(me, gain, weight, v_map, s_map, streams, n_sa):
    tokens = streams[0].shape[0]
    width, own = weight.shape

    def body(*refs):
        finish_body(n_sa, *refs)

    return pl.pallas_call(
        body,
        in_specs=[SCALARS] + [WHOLE] * (4 + len(streams)),
        out_specs=[WHOLE] * n_sa,
        out_shape=[jax.ShapeDtypeStruct((tokens, own), BF16)] * n_sa,
        scratch_shapes=[
            pltpu.VMEM((n_sa * tokens, width), BF16),
            pltpu.VMEM((n_sa, tokens, own), BF16),
        ],
        name="finish",
    )(me, gain, weight, v_map, s_map, *streams)


def place_body(me_ref, *refs):
    got, out_ref = refs[:-1], refs[-1]
    own = got[0].shape[1]
    for s, ref in enumerate(got):
        at = lax.rem(me_ref[0] - s + len(got), len(got))
        out_ref[:, pl.ds(pl.multiple_of(at * own, own), own)] = ref[...]


def key_arguments(qk, extra, tokens):
    n_sa = qk.shape[0]
    heads = HV // n_sa
    rates = qk[:, tokens : tokens + extra].reshape(n_sa, 3, 2 * heads, tokens).astype(F32)
    rates = rates[:, 0] + rates[:, 1] + rates[:, 2]
    qk = qk[:, :tokens]
    until = (
        lax.broadcasted_iota(jnp.int32, (tokens, tokens), 0)
        <= lax.broadcasted_iota(jnp.int32, (tokens, tokens), 1)
    ).astype(F32)
    sum_row = jnp.einsum("nhp,pt->nht", rates[:, :heads], until, precision=HIGHEST)
    rate_row = rates[:, heads:]
    half = qk.shape[2] // 2
    return (
        qk[..., :half],
        qk[..., half:],
        sum_row.transpose(0, 2, 1),
        sum_row,
        rate_row.transpose(0, 2, 1),
        rate_row,
    )


def on_device(
    expert_hidden,
    down_weight,
    residual,
    expert_ids,
    combine_weight,
    norm_gain,
    value_weight,
    queries,
    keys,
    log_decay,
    write_rate,
):
    n_z, n_x, n_c, n_sa = (lax.axis_size(a) for a in ("z", "x", "c", "sa"))
    n_xc = n_x * n_c
    exp_dev, _, width = down_weight.shape
    tokens = residual.shape[1]
    top = expert_ids.shape[2]
    own = width // n_sa
    heads = HV // n_sa
    sa = lax.axis_index("sa")
    me = sa[None]

    hidden = ordered_hidden(expert_hidden, n_z, n_xc)
    made = produce(hidden, down_weight, 0, CHUNKS[0], n_xc)

    table = jnp.concatenate([expert_ids[0].astype(F32), combine_weight[0]], axis=1).T
    table = after(table.astype(BF16), made).reshape(-1, own)
    part = lax.dynamic_slice_in_dim(value_weight, sa * own, own, axis=1)
    rows, extra = part.shape[0], table.shape[0]
    packed = jnp.concatenate([part, table, jnp.zeros((-extra % 8, own), BF16)], axis=0)
    packed = gathered(packed, "z", -1)
    part = packed[:, :rows]
    tables = packed[:, rows : rows + extra].reshape(n_z, 2 * top, tokens).astype(F32)
    combine = combine_matrix(tables.transpose(0, 2, 1), top, exp_dev, n_xc)

    def by_group(array):
        return array[0].reshape(tokens, n_sa, -1).transpose(1, 0, 2)

    log_decay, write_rate, queries, keys = lax.optimization_barrier(
        (log_decay, write_rate, queries, keys, made)
    )[:4]
    rates = jnp.concatenate(
        [log_decay[0].T.reshape(n_sa, heads, tokens), write_rate[0].T.reshape(n_sa, heads, tokens)],
        axis=1,
    )
    rates = jnp.stack(thirds(rates), axis=1).reshape(n_sa, -1, own)
    extra = rates.shape[1]
    rates = jnp.pad(rates, ((0, 0), (0, -extra % 8), (0, 0)))
    sent = jnp.concatenate([by_group(queries), by_group(keys)], axis=2)
    sent = jnp.concatenate([sent, rates], axis=1)
    qk = []
    for s in range(n_sa):
        piece = lax.dynamic_index_in_dim(sent, (sa + s) % n_sa, keepdims=False)
        qk.append(shifted(piece, "sa", s) if s else piece)
    qk = jnp.stack(qk)

    starts = [sum(CHUNKS[:n]) for n in range(len(CHUNKS))]

    def add_up(number, parts):
        own_part = residual[0, :, starts[number] : starts[number] + CHUNKS[number]]
        return sum_rounded(own_part, *parts)

    def spread(stream):
        return [stream] + [shifted(stream, "sa", s) for s in range(1, n_sa)]

    def exchange(rows):
        return lax.all_to_all(rows, ("x", "c"), split_axis=0, concat_axis=0, tiled=True)

    def make(rows, number):
        return produce(rows, down_weight, starts[number], CHUNKS[number], n_xc)

    def gather_chunk(weighting, rows):
        return combine_rows(weighting, rows, n_z, False)

    got = exchange(made)
    made = make(hidden, 1)
    v_map, s_map = key_maps(*key_arguments(qk, extra, tokens))
    made, v_map, s_map, got = lax.optimization_barrier((made, v_map, s_map, got))

    arrived = exchange(made)
    parts = gather_chunk(combine, got)
    first = start_sum_over_z(parts, True)
    made = make(after(hidden, parts[0]), 2)
    _, earlier = pass_on(*first, made)
    made, got = lax.optimization_barrier((made, arrived))

    arrived = exchange(made)
    parts = gather_chunk(combine, got)
    first = start_sum_over_z(parts, False)
    *earlier, _ = lax.optimization_barrier((*earlier, parts[0]))
    stream = add_up(0, earlier)
    streams = spread(stream)
    sums, earlier = pass_on(*first, stream)
    combine, *_ = lax.optimization_barrier((combine, *sums))

    parts = gather_chunk(combine, arrived)
    first = start_sum_over_z(parts, True)
    *earlier, _ = lax.optimization_barrier((*earlier, parts[0]))
    _, latest = pass_on(*first, parts[0])
    streams += spread(add_up(1, earlier))
    part = after(part, parts[0])
    part = jnp.stack([part] + [shifted(part, "x", r) for r in range(1, n_x)])
    streams += spread(add_up(2, latest))
    other = shifted(part, "c", 1)
    place = jnp.stack([lax.axis_index(a) for a in ("z", "x", "c")])
    projection = pl.pallas_call(
        order_body,
        in_specs=[SCALARS, WHOLE, WHOLE],
        out_specs=WHOLE,
        out_shape=jax.ShapeDtypeStruct((width, own), BF16),
        name="order",
    )(place, part, other)
    outs = finish(me, norm_gain[None], projection, v_map, s_map, streams, n_sa)
    outs = [outs[0]] + [shifted(outs[s], "sa", s) for s in range(1, n_sa)]
    out = pl.pallas_call(
        place_body,
        in_specs=[SCALARS] + [WHOLE] * n_sa,
        out_specs=WHOLE,
        out_shape=jax.ShapeDtypeStruct((tokens, width), BF16),
        name="place",
    )(me, *outs)
    return out[None]


def solution(mesh):
    fine = Mesh(mesh.devices.reshape(8, 4, 2, 4), ("z", "x", "c", "sa"))
    ea = ("z", "x", "c")
    return jax.shard_map(
        on_device,
        mesh=fine,
        in_specs=(
            P(ea, "sa", None),
            P(ea, None, None),
            P(ea, "sa", None),
            P(ea, "sa", None),
            P(ea, "sa", None),
            P(),
            P(ea, None),
            P(ea, "sa", None),
            P(ea, "sa", None),
            P(ea, "sa", None),
            P(ea, "sa", None),
        ),
        out_specs=P(ea, "sa", None),
        check_vma=False,
    )
```
